32 devices in a mesh: groups: 2 (over y), rows: 16 (over z, x, core).
Axes of the slice: x: 2, y: 2, z: 4, core: 2. Of those that a mesh axis runs over, the one named last changes fastest.
Arguments:
- pair_repr: bfloat16 [256, 128, 128], P('groups', 'rows'), parts along dimension 0, may hold values from -6 to 6
- single_repr: bfloat16 [256, 384], P(('groups', 'rows')), parts along dimension 0, may hold values from -6 to 6
- residue_index: int32 [256], P('groups'), parts along dimension 0, may hold values from 0 to 47
- chain_index: int32 [256], P('groups'), parts along dimension 0, may hold values from 0 to 3
- complex_index: int32 [256], P('groups'), parts along dimension 0, may hold values from 0 to 7, never falling along the last dimension, each value on 1 to 96 neighbouring positions
- pad_mask: int32 [256], P('groups'), parts along dimension 0, may hold values 0 or 1
- w_query: bfloat16 [384, 384], replicated, may hold values from -3 to 3
- w_key: bfloat16 [384, 384], replicated, may hold values from -3.1 to 3.1
- w_value: bfloat16 [384, 384], replicated, may hold values from -0.3125 to 0.3125
- w_gate: bfloat16 [384, 384], replicated, may hold values from -0.3125 to 0.3125
- w_out: bfloat16 [384, 384], replicated, may hold values from -2.5 to 2.5
- w_bias: bfloat16 [128, 16], replicated, may hold values from -0.5 to 0.5
- rel_table: bfloat16 [66, 128], replicated, may hold values from -6 to 6
- w_mix_a: bfloat16 [384, 128], replicated, may hold values from -0.3125 to 0.3125
- w_mix_b: bfloat16 [384, 128], replicated, may hold values from -0.3125 to 0.3125
- w_hidden_a: bfloat16 [128, 512], replicated, may hold values from -0.5 to 0.5
- w_hidden_b: bfloat16 [128, 512], replicated, may hold values from -0.5 to 0.5
- w_hidden_out: bfloat16 [512, 128], replicated, may hold values from -0.25 to 0.25
- w_pae: bfloat16 [128, 64], replicated, may hold values from -30 to 30
- pae_bias: float32 [64], replicated, may hold values from -4 to 4
Outputs:
- refined: bfloat16 [256, 384], P(('groups', 'rows')), parts along dimension 0
- errors: float32 [256, 128], P(('groups', 'rows')), parts along dimension 0
The draws below stay inside these ranges and needn't reach their ends.
There are 2 independent parts, one for each index of `groups`. The reference program is written for one: setup_inputs(seed, part) draws one part's arguments, and reference() takes and returns one part's arrays. A program takes and returns all parts, laid end to end along the dimension named above; an argument that names none is the same for every part. Nothing has to cross between parts.
Inputs may be any that keep to these rules, and one draw needn't show every extreme that they name: `complex_index`: never falls along the tokens; each complex holds 1 to 96 consecutive tokens.
All inputs are finite; a program needn't handle non-finite values.
Results may differ from the reference program's by a relative error of at most 0.023.
Values may be sent and summed in bfloat16 or wider, within the bound.
A program may use at most 128 MiB of HBM per device.

```python
import math
import jax
import jax.numpy as jnp
import numpy as np
from jax import lax

C = 128
S = 384
HEADS = 16
BINS = 64
FFN = 512
TOK_DEV = 8
N = 128
REL_BINS = 66


def query_key_pair(key):
    base = jax.random.normal(jax.random.fold_in(key, 101), (S, S), jnp.float32)
    other = jax.random.normal(jax.random.fold_in(key, 202), (S, S), jnp.float32)
    return (jnp.clip(base, -6.0, 6.0) * (2.0 * S ** (-0.5)), jnp.clip(other, -6.0, 6.0) * (2.0 * S ** (-0.5)))


def draw_w_query(key, part):
    return query_key_pair(key)[0].astype(jnp.bfloat16)


def draw_w_key(key, part):
    return query_key_pair(key)[1].astype(jnp.bfloat16)


def draw_w_pae(key, part):
    base = jax.random.normal(jax.random.fold_in(key, 404), (C, BINS), jnp.float32)
    return (jnp.clip(base, -6.0, 6.0) * C ** (-0.5)).astype(jnp.bfloat16)


def plant(array, own_key, least, largest):
    longest = array.shape.index(max(array.shape))
    spots = []
    for shift in (0, 1):
        where = [jax.random.randint(jax.random.fold_in(own_key, axis), (), 0, length) for axis, length in enumerate(array.shape)]
        where[longest] = (where[longest] + shift) % array.shape[longest]
        spots.append(tuple(where))
    return array.at[spots[0]].set(least).at[spots[1]].set(largest)


def shard_levels(own_key, dims, pieces, low, high):
    level = 1.0
    for position, parts in pieces:
        draws = jax.random.uniform(jax.random.fold_in(jax.random.fold_in(own_key, 6), position), (parts,), jnp.float32, low / len(pieces), high / len(pieces))
        level = level * jnp.repeat(jnp.exp(draws), dims[position] // parts).reshape((-1,) + (1,) * (len(dims) - 1 - position))
    return level


def split_up(count, total, most, slope):
    loads = [(1 << 20) // math.isqrt(standing ** slope) + 1 for standing in range(2, count + 1)]
    surplus, counts = total - most - (count - 1), [1] * (count - 1)
    while surplus > 0:
        candidates = [i for i in range(count - 1) if counts[i] < most]
        mass, remaining = sum([loads[i] for i in candidates]), surplus
        for i in candidates:
            addition = min(most - counts[i], max(1, remaining * loads[i] // mass), surplus)
            counts[i] = counts[i] + addition
            surplus = surplus - addition
    return np.array([most] + counts)


def ragged_sizes(own_key, amount, total, most, lean):
    if amount == 2:
        one = jax.random.randint(own_key, (), max(1, total - most), min(most, total - 1) + 1)
        return jnp.stack([one, total - one])
    sizes = jnp.asarray(split_up(amount, total, most, lean), jnp.int32)
    twos = (amount - 1) // 2
    giver, receiver = sizes[1:1 + 2 * twos:2], sizes[2:2 + 2 * twos:2]
    margin = jnp.minimum(giver - 1, most - receiver)
    moved = jax.random.randint(jax.random.fold_in(own_key, 1), (twos,), 0, 1 << 20) % (margin + 1)
    sizes = sizes.at[1:1 + 2 * twos:2].set(giver - moved).at[2:2 + 2 * twos:2].set(receiver + moved)
    return sizes[jax.random.permutation(jax.random.fold_in(own_key, 2), amount)]


def gaussian(stream_key, shape, scale, most, shards=(), kind=jnp.bfloat16):
    gain = shard_levels(stream_key, shape, shards, -0.22, 0.18) if shards else 1.0
    array = jax.random.normal(stream_key, shape, jnp.float32) * scale * gain
    return jnp.minimum(jnp.maximum(array, -most), most).astype(kind)


def setup_inputs(seed: int = 0, part: int = 0) -> dict:
    streams_of = jax.random.split(jax.random.key(seed), 21)
    part_splits = jax.random.split(jax.random.fold_in(streams_of[20], part), 21)
    pair_repr = gaussian(part_splits[0], (N, N, C), 1.0, 6.0, ((1, 16),))
    single_repr = gaussian(part_splits[1], (N, S), 1.0, 6.0, ((0, 16),))
    residue_index = plant(jax.random.randint(part_splits[2], (N,), 0, 48), jax.random.fold_in(part_splits[2], 1), 0, 47).astype(jnp.int32)
    chain_index = plant(jax.random.randint(part_splits[3], (N,), 0, 4), jax.random.fold_in(part_splits[3], 1), 0, 3).astype(jnp.int32)
    complex_index = jnp.searchsorted(jnp.cumsum(ragged_sizes(part_splits[4], 8, N, 3 * N // 4, 1)), jnp.arange(N), side="right").astype(jnp.int32)
    pad_mask = plant((jax.random.randint(part_splits[5], (N,), 0, 8) < 7).astype(jnp.int32), jax.random.fold_in(part_splits[5], 1), 0, 1)
    w_query = draw_w_query(jax.random.fold_in(streams_of[20], 71), part)
    w_key = draw_w_key(jax.random.fold_in(streams_of[20], 71), part)
    w_value = gaussian(streams_of[8], (S, S), S ** -0.5, 0.3125)
    w_gate = gaussian(streams_of[9], (S, S), S ** -0.5, 0.3125)
    w_out = gaussian(streams_of[10], (S, S), (max(S // 64, 1)) ** -0.5, 2.5)
    w_bias = gaussian(streams_of[11], (C, HEADS), C ** -0.5, 0.5)
    rel_table = gaussian(streams_of[12], (REL_BINS, C), 1.0, 6.0)
    w_mix_a = gaussian(streams_of[13], (S, C), S ** -0.5, 0.3125)
    w_mix_b = gaussian(streams_of[14], (S, C), S ** -0.5, 0.3125)
    w_hidden_a = gaussian(streams_of[15], (C, FFN), C ** -0.5, 0.5)
    w_hidden_b = gaussian(streams_of[16], (C, FFN), C ** -0.5, 0.5)
    w_hidden_out = gaussian(streams_of[17], (FFN, C), FFN ** -0.5, 0.25)
    w_pae = draw_w_pae(jax.random.fold_in(streams_of[20], 71), part)
    pae_bias = gaussian(streams_of[19], (BINS,), 1.0, 4.0, (), jnp.float32)
    return dict(pair_repr=pair_repr, single_repr=single_repr, residue_index=residue_index, chain_index=chain_index, complex_index=complex_index, pad_mask=pad_mask, w_query=w_query, w_key=w_key, w_value=w_value, w_gate=w_gate, w_out=w_out, w_bias=w_bias, rel_table=rel_table, w_mix_a=w_mix_a, w_mix_b=w_mix_b, w_hidden_a=w_hidden_a, w_hidden_b=w_hidden_b, w_hidden_out=w_hidden_out, w_pae=w_pae, pae_bias=pae_bias)


epsilon = 1e-05
masked_score = -1e+30

def norm_rows(values):
    center = values - lax.optimization_barrier(jnp.mean(values, axis=-1, keepdims=True))
    spread = lax.optimization_barrier(jnp.mean(center * center, axis=-1, keepdims=True))
    return center * lax.rsqrt(spread + epsilon)

def relative(res_query, chain_query, res_key, chain_key, rel_table):
    reach = (rel_table.shape[0] - 2) // 2
    offsets = jnp.clip(res_query[:, None] - res_key[None, :], -reach, reach) + reach
    bucket = jnp.where(chain_query[:, None] == chain_key[None, :], offsets, 2 * reach + 1)
    classes = jnp.arange(rel_table.shape[0], dtype=jnp.int32)
    onehot = (bucket[:, :, None] == classes[None, None, :]).astype(jnp.float32)
    return jnp.einsum('qkr,rc->qkc', onehot, rel_table.astype(jnp.float32))

def pair_tail(mixed, w_hidden_a, w_hidden_b, w_hidden_out, w_pae, pae_bias):
    width = mixed.shape[-1]
    flat = mixed.reshape(-1, width)
    normed = norm_rows(flat).astype(jnp.bfloat16)
    gate_part = jnp.dot(normed, w_hidden_a, preferred_element_type=jnp.float32)
    up_part = jnp.dot(normed, w_hidden_b, preferred_element_type=jnp.float32)
    hidden = (jax.nn.silu(gate_part) * up_part).astype(jnp.bfloat16)
    updated = flat + jnp.dot(hidden, w_hidden_out, preferred_element_type=jnp.float32)
    final = norm_rows(updated).astype(jnp.bfloat16)
    logits = jnp.dot(final, w_pae, preferred_element_type=jnp.float32) + pae_bias.astype(jnp.float32)[None, :]
    probs = jax.nn.softmax(logits, axis=-1)
    bins = w_pae.shape[1]
    centers = (jnp.arange(bins, dtype=jnp.float32) + 0.5) * (32.0 / bins)
    return lax.optimization_barrier(jnp.sum(probs * centers[None, :], axis=-1)).reshape(mixed.shape[:-1])

def reference(pair_repr, single_repr, residue_index, chain_index, complex_index, pad_mask, w_query, w_key, w_value, w_gate, w_out, w_bias, rel_table, w_mix_a, w_mix_b, w_hidden_a, w_hidden_b, w_hidden_out, w_pae, pae_bias):
    total_rows = single_repr.shape[0]
    head_count = w_bias.shape[1]
    head_size = single_repr.shape[1] // head_count
    block_rows = TOK_DEV
    normed = norm_rows(single_repr.astype(jnp.float32)).astype(jnp.bfloat16)
    queries = jnp.dot(normed, w_query, preferred_element_type=jnp.float32).astype(jnp.bfloat16)
    keys_all = jnp.dot(normed, w_key, preferred_element_type=jnp.float32).astype(jnp.bfloat16)
    values_all = jnp.dot(normed, w_value, preferred_element_type=jnp.float32).astype(jnp.bfloat16)
    gating = jax.nn.sigmoid(jnp.dot(normed, w_gate, preferred_element_type=jnp.float32))
    token_ids = jnp.arange(total_rows, dtype=jnp.int32)
    key_heads = keys_all.astype(jnp.float32).reshape(total_rows, head_count, head_size)
    value_heads = values_all.astype(jnp.float32).reshape(total_rows, head_count, head_size)

    def pair_input(offset):
        rows_pair = lax.dynamic_slice_in_dim(pair_repr, offset, block_rows, 0).astype(jnp.float32)
        res_rows = lax.dynamic_slice_in_dim(residue_index, offset, block_rows, 0)
        chain_rows = lax.dynamic_slice_in_dim(chain_index, offset, block_rows, 0)
        return rows_pair + relative(res_rows, chain_rows, residue_index, chain_index, rel_table)

    def attend(block):
        offset = (block * block_rows).astype(jnp.int32)
        pair_in = pair_input(offset)
        pair_bias = jnp.einsum('qkc,ch->hqk', norm_rows(pair_in).astype(jnp.bfloat16).astype(jnp.float32), w_bias.astype(jnp.float32)).astype(jnp.bfloat16)
        query_rows = lax.dynamic_slice_in_dim(queries, offset, block_rows, 0).astype(jnp.float32).reshape(block_rows, head_count, head_size)
        scores = jnp.einsum('qhd,khd->hqk', query_rows, key_heads) / math.sqrt(head_size) + pair_bias.astype(jnp.float32)
        row_ids = offset + jnp.arange(block_rows, dtype=jnp.int32)
        complex_rows = lax.dynamic_slice_in_dim(complex_index, offset, block_rows, 0)
        allowed = (complex_rows[:, None] == complex_index[None, :]) & ((pad_mask[None, :] == 1) | (row_ids[:, None] == token_ids[None, :]))
        scores = jnp.where(allowed[None], scores, masked_score)
        row_max = lax.optimization_barrier(jnp.max(scores, axis=-1, keepdims=True))
        expo = jnp.exp(scores - row_max)
        row_sum = lax.optimization_barrier(jnp.sum(expo, axis=-1))
        rounded = expo.astype(jnp.bfloat16).astype(jnp.float32)
        output = jnp.einsum('hqk,khd->hqd', rounded, value_heads) / row_sum[..., None]
        return output.transpose(1, 0, 2).reshape(block_rows, head_count * head_size)
    block_count = total_rows // block_rows
    attended = lax.map(attend, jnp.arange(block_count, dtype=jnp.int32)).reshape(total_rows, -1)
    refined = (single_repr.astype(jnp.float32) + jnp.dot((gating * attended).astype(jnp.bfloat16), w_out, preferred_element_type=jnp.float32)).astype(jnp.bfloat16)
    renormed = norm_rows(refined.astype(jnp.float32)).astype(jnp.bfloat16)
    factor_a = jnp.dot(renormed, w_mix_a, preferred_element_type=jnp.float32).astype(jnp.bfloat16)
    factor_b = jnp.dot(renormed, w_mix_b, preferred_element_type=jnp.float32).astype(jnp.bfloat16)

    def finish(block):
        offset = (block * block_rows).astype(jnp.int32)
        pair_in = pair_input(offset)
        rows_a = lax.dynamic_slice_in_dim(factor_a, offset, block_rows, 0).astype(jnp.float32)
        mixed = pair_in + rows_a[:, None, :] * factor_b.astype(jnp.float32)[None, :, :]
        return pair_tail(mixed, w_hidden_a, w_hidden_b, w_hidden_out, w_pae, pae_bias)
    errors = lax.map(finish, jnp.arange(block_count, dtype=jnp.int32)).reshape(total_rows, total_rows)
    return (refined, errors)
```

```python
import functools
import math

import jax
import jax.numpy as jnp
from jax import lax
from jax.experimental import pallas as pl
from jax.experimental.pallas import tpu as pltpu
from jax.sharding import PartitionSpec as P

epsilon = 1e-05
masked_score = -1e30
chain_step = 65536.0
f32 = jnp.float32
bf16 = jnp.bfloat16


def norm_rows(values):
    center = values - jnp.mean(values, axis=-1, keepdims=True)
    spread = jnp.mean(center * center, axis=-1, keepdims=True)
    return center * lax.rsqrt(spread + epsilon)


def mm(a, b):
    return jnp.dot(a, b, preferred_element_type=f32)


def mm_nt(a, b):
    return lax.dot_general(a, b, (((1,), (1,)), ((), ())), preferred_element_type=f32)


def mm_tn(a, b):
    return lax.dot_general(a, b, (((0,), (0,)), ((), ())), preferred_element_type=f32)


def column(row):
    m = row.shape[1]
    pick = lax.broadcasted_iota(jnp.int32, (m, m), 0) == lax.broadcasted_iota(jnp.int32, (m, m), 1)
    return jnp.sum(jnp.where(pick, row, 0.0), axis=1, keepdims=True)


def bucket_onehot(diff, classes):
    reach = (classes - 2) // 2
    same = jnp.abs(diff) < 0.5 * chain_step
    bucket = jnp.where(same, jnp.clip(diff, -reach, reach) + reach, 2.0 * reach + 1.0)
    lanes = lax.broadcasted_iota(jnp.int32, bucket.shape, bucket.ndim - 1).astype(f32)
    return jnp.where(bucket == lanes, 1.0, 0.0).astype(bf16)


def kernel(
    n,
    heads,
    pair_h, single_h, res_h, chain_h, complex_h, pad_h,
    wq_h, wk_h, wv_h, wg_h, wo_h, wb_h, rel_h, wma_h, wmb_h, wha_h, whb_h, who_h, wp_h, pb_h,
    refined_ref, errors_ref,
    pair_v, single_v, res_v, chain_v, complex_v, pad_v,
    wq_v, wk_v, wv_v, wg_v, wo_v, wb_v, rel_v, wma_v, wmb_v, wha_v, whb_v, who_v, wp_v, pb_v,
    code_v, ccol_v, mask_v, bias_s, bias_r, norm_s, norm_r, pair_r, b_s, b_r, a_v, pin_v,
    flat_v, x_v, hid_v,
    local_sem, send_sem, recv_sem,
):
    me = lax.axis_index("rows")
    count, rows, width = pair_h.shape
    classes = rel_h.shape[0]
    inner = single_h.shape[1]
    head_size = inner // heads
    spots = rows * heads
    first = pl.multiple_of(me * rows, rows)
    step = min(count, 128)
    short = count == step

    hbm = (pair_h, single_h, res_h, chain_h, complex_h, pad_h, wq_h, wk_h, wv_h, wg_h, wo_h,
           wb_h, rel_h, wma_h, wmb_h, wha_h, whb_h, who_h, wp_h, pb_h)
    vmem = (pair_v, single_v, res_v, chain_v, complex_v, pad_v, wq_v, wk_v, wv_v, wg_v, wo_v,
            wb_v, rel_v, wma_v, wmb_v, wha_v, whb_v, who_v, wp_v, pb_v)
    (PAIR, SINGLE, RES, CHAIN, COMPLEX, PAD, WQ, WK, WV, WG, WO, WB, REL, WMA, WMB, WHA, WHB,
     WHO, WP, PB) = range(len(hbm))
    loads = [pltpu.make_async_copy(h, v, local_sem.at[i]) for i, (h, v) in enumerate(zip(hbm, vmem))]

    def arrive(*which):
        for i in which:
            loads[i].wait()

    bits = n.bit_length() - 1
    flips = [(1 << b) * (1 - 2 * ((me // (1 << b)) % 2)) for b in range(bits)]

    def each_peer(visit):
        if short and n == 1 << bits:
            for s in reversed(range(1, n)):
                visit(me + sum(flips[b] for b in range(bits) if s >> b & 1))
        else:
            def body(s, _):
                visit(lax.rem(me + s, n))
                return 0

            lax.fori_loop(1, n, body, 0)

    for i in (RES, CHAIN, SINGLE):
        loads[i].start()
    barrier = pltpu.get_barrier_semaphore()
    each_peer(lambda peer: pl.semaphore_signal(
        barrier, inc=1, device_id={"rows": peer}, device_id_type=pl.DeviceIdType.MESH))
    for i in (REL, WB, PAIR, COMPLEX, PAD, WQ, WG, WK, WV, WO, WMB, WMA, WHA, WHB, WHO, WP, PB):
        loads[i].start()

    arrive(RES, CHAIN)
    for k in range(0, count, step):
        code = chain_v[:, k:k + step].astype(f32) * chain_step + res_v[:, k:k + step].astype(f32)
        code_v[k:k + step, :] = jnp.broadcast_to(column(code), (step, 128))

    arrive(SINGLE)
    mine = single_v[...].astype(f32)
    normed = norm_rows(mine).astype(bf16)
    norm_s[...] = normed
    norm_r[me] = normed

    arrive(REL, WB, PAIR)
    rel = rel_v[...]
    tile_h = jnp.where(
        lax.broadcasted_iota(jnp.int32, (heads, spots), 1) % heads
        == lax.broadcasted_iota(jnp.int32, (heads, spots), 0), 1.0, 0.0).astype(bf16)
    w_tiled = mm_tn(wb_v[...], tile_h).astype(bf16)
    code_keys = code_v[pl.ds(first, rows), :classes]

    def bias_block(j, _):
        at = pl.multiple_of(j * step, step)
        code_i = code_v[pl.ds(at, step), :classes]
        diff = code_i[:, None, :] - code_keys[None, :, :]
        hot = bucket_onehot(diff.reshape(step * rows, classes), classes)
        cells = mm(hot, rel) + pair_v[pl.ds(at, step)].astype(f32).reshape(step * rows, width)
        out = mm(norm_rows(cells).astype(bf16), w_tiled)
        out = out.reshape(step // rows, rows, rows, spots)
        lane_q = lax.broadcasted_iota(jnp.int32, (1, 1, spots), 2) // heads
        total = jnp.where(lane_q == 0, out[:, 0], 0.0)
        for q in range(1, rows):
            total = jnp.where(lane_q == q, out[:, q], total)
        bias_s[pl.ds(pl.multiple_of(j * (step // rows), step // rows), step // rows)] = total.astype(bf16)
        return 0

    lax.fori_loop(0, count // step, bias_block, 0, unroll=short)
    bias_r[me] = bias_s[me]

    pl.semaphore_wait(barrier, n - 1)

    def remote(src, dst, i, peer):
        return pltpu.make_async_remote_copy(
            src_ref=src, dst_ref=dst, send_sem=send_sem.at[i], recv_sem=recv_sem.at[i],
            device_id={"rows": peer}, device_id_type=pl.DeviceIdType.MESH)

    each_peer(lambda peer: remote(norm_s, norm_r.at[me], 0, peer).start())
    each_peer(lambda peer: remote(bias_s.at[peer], bias_r.at[me], 1, peer).start())

    arrive(WQ)
    queries = mm(normed, wq_v[...]).astype(bf16).astype(f32)
    arrive(WG)
    gating = jax.nn.sigmoid(mm(normed, wg_v[...]))
    head_of = lax.broadcasted_iota(jnp.int32, (heads, inner), 1) // head_size
    own_head = head_of == lax.broadcasted_iota(jnp.int32, (heads, inner), 0)
    q_wide = jnp.concatenate(
        [jnp.where(own_head, queries[q:q + 1, :], 0.0) for q in range(rows)], axis=0).astype(bf16)
    arrive(WK)
    toward = (mm_nt(wk_v[...], q_wide) / math.sqrt(head_size)).astype(bf16)

    each_peer(lambda peer: remote(
        pair_v.at[pl.ds(peer * rows, rows)], pair_r.at[me], 2, peer).start())
    pair_r[me] = pair_v[pl.ds(first, rows)]

    arrive(COMPLEX, PAD)
    lane_spot = lax.broadcasted_iota(jnp.int32, (step, spots), 1) // heads
    for k in range(0, count, step):
        ccol_v[k:k + step, :] = jnp.broadcast_to(
            column(complex_v[:, k:k + step].astype(f32)), (step, 128))
    mine_c = ccol_v[pl.ds(first, rows), 0:1]
    lane_row = lax.broadcasted_iota(jnp.int32, (rows, spots), 1) // heads
    pick = lane_row == lax.broadcasted_iota(jnp.int32, (rows, spots), 0)
    query_c = jnp.sum(jnp.where(pick, mine_c, 0.0), axis=0, keepdims=True)
    for k in range(0, count, step):
        real = column(pad_v[:, k:k + step].astype(f32)) == 1.0
        same = ccol_v[k:k + step, :spots] == query_c
        itself = (lax.broadcasted_iota(jnp.int32, (step, spots), 0) + k) == (first + lane_spot)
        mask_v[k:k + step, :] = jnp.where(same & (real | itself), 0.0, masked_score)

    def rel_block(q, _):
        diff = code_v[pl.ds(first + q, 1), :classes] - code_v[:, :classes]
        pin_v[q] = mm(bucket_onehot(diff, classes), rel)
        return 0

    lax.fori_loop(0, rows, rel_block, 0, unroll=short)

    arrive(WHA, WHB, WHO, WP, PB)
    wha_v[...] = (wha_v[...].astype(f32) * 0.5).astype(bf16)
    bins = wp_v.shape[0]
    bias_col = column(pb_v[...])
    centers = (lax.broadcasted_iota(jnp.int32, (bins, 1), 0).astype(f32) + 0.5) * (32.0 / bins)
    arrive(WV, WO, WMB, WMA)

    landed = norm_r.at[pl.ds(0, n - 1)]
    pltpu.make_async_copy(landed, landed, recv_sem.at[0]).wait()
    every = norm_r[...].astype(f32).reshape(count, inner).astype(bf16)
    scores = mm(every, toward)
    values = mm(every, wv_v[...]).astype(bf16)
    landed = bias_r.at[pl.ds(0, n - 1)]
    pltpu.make_async_copy(landed, landed, recv_sem.at[1]).wait()
    scores = scores + bias_r[...].astype(f32).reshape(count, spots) + mask_v[...]
    expo = jnp.exp(scores - jnp.max(scores, axis=0, keepdims=True))
    weights = (expo * (1.0 / jnp.sum(expo, axis=0, keepdims=True))).astype(bf16)
    mixed_heads = mm_tn(weights, values)
    attended = jnp.concatenate(
        [jnp.sum(jnp.where(own_head, mixed_heads[q * heads:(q + 1) * heads, :], 0.0),
                 axis=0, keepdims=True) for q in range(rows)], axis=0)
    refined = (mine + mm((gating * attended).astype(bf16), wo_v[...])).astype(bf16)
    renormed = norm_rows(refined.astype(f32)).astype(bf16)
    factor_b = mm(renormed, wmb_v[...]).astype(bf16)
    b_s[...] = factor_b
    a_v[...] = mm(renormed, wma_v[...]).astype(bf16).astype(f32)
    b_r[me] = factor_b
    refined_ref[...] = refined

    each_peer(lambda peer: remote(b_s, b_r.at[me], 3, peer).start())

    landed = pair_r.at[pl.ds(0, n - 1)]
    pltpu.make_async_copy(landed, landed, recv_sem.at[2]).wait()

    def add_block(q, _):
        pin_v[q] = pin_v[q] + pair_r[:, q].astype(f32).reshape(count, width)
        return 0

    lax.fori_loop(0, rows, add_block, 0, unroll=short)

    landed = b_r.at[pl.ds(0, n - 1)]
    pltpu.make_async_copy(landed, landed, recv_sem.at[3]).wait()

    def tail(c, _):
        at = pl.multiple_of(c * step, step)
        tile = pl.multiple_of(c * (step // rows), step // rows)
        factor_b = b_r[pl.ds(tile, step // rows)].astype(f32).reshape(step, width)
        for q in range(rows):
            flat = pin_v[q, pl.ds(at, step), :] + a_v[q:q + 1, :] * factor_b
            flat_v[q * step:(q + 1) * step, :] = flat
            x_v[q * step:(q + 1) * step, :] = norm_rows(flat).astype(bf16)
        cut = 256
        for k in range(0, wha_v.shape[1], cut):
            wa = wha_v[:, k:k + cut]
            wb = whb_v[:, k:k + cut]
            for q in range(rows):
                x = x_v[q * step:(q + 1) * step, :]
                half = mm(x, wa)
                up = mm(x, wb)
                hid_v[q * step:(q + 1) * step, k:k + cut] = (
                    (half + half * jnp.tanh(half)) * up).astype(bf16)
        for q in range(rows):
            updated = flat_v[q * step:(q + 1) * step, :] + mm(hid_v[q * step:(q + 1) * step, :], who_v[...])
            x_v[q * step:(q + 1) * step, :] = norm_rows(updated).astype(bf16)
        found = []
        for q in range(rows):
            logits = mm_nt(wp_v[...], x_v[q * step:(q + 1) * step, :]) + bias_col
            expo = jnp.exp(logits - jnp.max(logits, axis=0, keepdims=True))
            found.append(jnp.sum(expo * centers, axis=0, keepdims=True)
                         / jnp.sum(expo, axis=0, keepdims=True))
        errors_ref[:, pl.ds(at, step)] = jnp.concatenate(found, axis=0)
        return 0

    lax.fori_loop(0, count // step, tail, 0, unroll=short)

    for i, buf in enumerate((norm_r, bias_r, pair_r, b_r)):
        sent = buf.at[pl.ds(0, n - 1)]
        pltpu.make_async_copy(sent, sent, send_sem.at[i]).wait()


def place(refined_v, errors_v, refined_h, errors_h, sem):
    copies = (
        pltpu.make_async_copy(refined_v, refined_h, sem.at[0]),
        pltpu.make_async_copy(errors_v, errors_h, sem.at[1]),
    )
    for copy in copies:
        copy.start()
    for copy in copies:
        copy.wait()


def on_device(n, pair_repr, single_repr, residue_index, chain_index, complex_index, pad_mask,
              w_query, w_key, w_value, w_gate, w_out, w_bias, rel_table, w_mix_a, w_mix_b,
              w_hidden_a, w_hidden_b, w_hidden_out, w_pae, pae_bias):
    count, rows, width = pair_repr.shape
    inner = single_repr.shape[1]
    heads = w_bias.shape[1]
    hidden = w_hidden_a.shape[1]
    args = (pair_repr, single_repr, residue_index[None], chain_index[None], complex_index[None],
            pad_mask[None], w_query, w_key, w_value, w_gate, w_out, w_bias.T, rel_table,
            w_mix_a, w_mix_b, w_hidden_a, w_hidden_b, w_hidden_out, w_pae.T, pae_bias[None])
    spots = rows * heads
    step = min(count, 128)
    scratch = [pltpu.VMEM(a.shape, a.dtype) for a in args] + [
        pltpu.VMEM((count, 128), f32),
        pltpu.VMEM((count, 128), f32),
        pltpu.VMEM((count, spots), f32),
        pltpu.VMEM((n, rows, spots), bf16),
        pltpu.VMEM((n, rows, spots), bf16),
        pltpu.VMEM((rows, inner), bf16),
        pltpu.VMEM((n, rows, inner), bf16),
        pltpu.VMEM((n, rows, rows, width), bf16),
        pltpu.VMEM((rows, width), bf16),
        pltpu.VMEM((n, rows, width), bf16),
        pltpu.VMEM((rows, width), f32),
        pltpu.VMEM((rows, count, width), f32),
        pltpu.VMEM((rows * step, width), f32),
        pltpu.VMEM((rows * step, width), bf16),
        pltpu.VMEM((rows * step, hidden), bf16),
        pltpu.SemaphoreType.DMA((len(args),)),
        pltpu.SemaphoreType.DMA((4,)),
        pltpu.SemaphoreType.DMA((4,)),
    ]
    refined, errors = pl.pallas_call(
        functools.partial(kernel, n, heads),
        out_shape=(pltpu.VMEM((rows, inner), bf16), pltpu.VMEM((rows, count), f32)),
        in_specs=[pl.BlockSpec(memory_space=pltpu.HBM)] * len(args),
        out_specs=[pl.BlockSpec(memory_space=pltpu.VMEM)] * 2,
        scratch_shapes=scratch,
        compiler_params=pltpu.CompilerParams(
            collective_id=0, has_side_effects=True, vmem_limit_bytes=40 * 1024 * 1024),
        name="confidence",
    )(*[pltpu.with_memory_space_constraint(a, pltpu.HBM) for a in args])
    return pl.pallas_call(
        place,
        out_shape=(
            jax.ShapeDtypeStruct((rows, inner), bf16),
            jax.ShapeDtypeStruct((rows, count), f32),
        ),
        in_specs=[pl.BlockSpec(memory_space=pltpu.VMEM)] * 2,
        out_specs=[pl.BlockSpec(memory_space=pltpu.HBM)] * 2,
        scratch_shapes=[pltpu.SemaphoreType.DMA((2,))],
        compiler_params=pltpu.CompilerParams(vmem_limit_bytes=1024 * 1024),
        name="place",
    )(refined, errors)


def solution(mesh):
    placed = (
        P("groups", "rows", None),
        P(("groups", "rows"), None),
        P("groups"),
        P("groups"),
        P("groups"),
        P("groups"),
    ) + (P(),) * 14
    return jax.shard_map(
        functools.partial(on_device, mesh.shape["rows"]),
        mesh=mesh,
        in_specs=placed,
        out_specs=(P(("groups", "rows"), None), P(("groups", "rows"), None)),
        check_vma=False,
    )
```

```python
import functools
import math

import jax
import jax.numpy as jnp
from jax import lax
from jax.experimental import pallas as pl
from jax.experimental.pallas import tpu as pltpu
from jax.sharding import PartitionSpec as P

epsilon = 1e-05
masked_score = -1e30
chain_step = 65536.0
f32 = jnp.float32
bf16 = jnp.bfloat16


EARLY = (2, 1, 0)
LATE = (3,)
TRIGGER = 0
PIECES = (('a', (0, 1)), ('b', (2, 3)))


def norm_rows(values):
    center = values - jnp.mean(values, axis=-1, keepdims=True)
    spread = jnp.mean(center * center, axis=-1, keepdims=True)
    return center * lax.rsqrt(spread + epsilon)


def mm(a, b):
    return jnp.dot(a, b, preferred_element_type=f32)


def mm_nt(a, b):
    return lax.dot_general(a, b, (((1,), (1,)), ((), ())), preferred_element_type=f32)


def mm_tn(a, b):
    return lax.dot_general(a, b, (((0,), (0,)), ((), ())), preferred_element_type=f32)


def column(row):
    m = row.shape[1]
    pick = lax.broadcasted_iota(jnp.int32, (m, m), 0) == lax.broadcasted_iota(jnp.int32, (m, m), 1)
    return jnp.sum(jnp.where(pick, row, 0.0), axis=1, keepdims=True)


def bucket_onehot(diff, classes):
    reach = (classes - 2) // 2
    same = jnp.abs(diff) < 0.5 * chain_step
    bucket = jnp.where(same, jnp.clip(diff, -reach, reach) + reach, 2.0 * reach + 1.0)
    lanes = lax.broadcasted_iota(jnp.int32, bucket.shape, bucket.ndim - 1).astype(f32)
    return jnp.where(bucket == lanes, 1.0, 0.0).astype(bf16)


def kernel(
    n,
    heads,
    pair_h, single_h, res_h, chain_h, complex_h, pad_h,
    wq_h, wk_h, wv_h, wg_h, wo_h, wb_h, rel_h, wma_h, wmb_h, wha_h, whb_h, who_h, wp_h, pb_h,
    refined_ref, errors_ref,
    pair_v, single_v, res_v, chain_v, complex_v, pad_v,
    wq_v, wk_v, wv_v, wg_v, wo_v, wb_v, rel_v, wma_v, wmb_v, wha_v, whb_v, who_v, wp_v, pb_v,
    code_v, ccol_v, mask_v, bias_s, bias_r, norm_s, norm_r, pair_r, b_s, b_r, a_v, pin_v,
    flat_v, x_v, hid_v,
    local_sem, send_sem, recv_sem,
):
    me = lax.axis_index("rows")
    count, rows, width = pair_h.shape
    classes = rel_h.shape[0]
    inner = single_h.shape[1]
    head_size = inner // heads
    spots = rows * heads
    first = pl.multiple_of(me * rows, rows)
    step = min(count, 128)
    short = count == step
    sub = 32

    hbm = (pair_h, single_h, res_h, chain_h, complex_h, pad_h, wq_h, wk_h, wv_h, wg_h, wo_h,
           wb_h, rel_h, wma_h, wmb_h, wha_h, whb_h, who_h, wp_h, pb_h)
    vmem = (pair_v, single_v, res_v, chain_v, complex_v, pad_v, wq_v, wk_v, wv_v, wg_v, wo_v,
            wb_v, rel_v, wma_v, wmb_v, wha_v, whb_v, who_v, wp_v, pb_v)
    (PAIR, SINGLE, RES, CHAIN, COMPLEX, PAD, WQ, WK, WV, WG, WO, WB, REL, WMA, WMB, WHA, WHB,
     WHO, WP, PB) = range(len(hbm))
    loads = [pltpu.make_async_copy(h, v, local_sem.at[i]) for i, (h, v) in enumerate(zip(hbm, vmem))]

    def arrive(*which):
        for i in which:
            loads[i].wait()

    parts = 4 if n % 4 == 0 else 1
    size = n // parts
    mine_at = me % size
    group = me // size
    low = group % 2
    groups = (group, group + 1 - 2 * low, group + 2 - 4 * (group // 2), 3 - group)[:parts]
    span = size * rows

    def each_peer(k, visit):
        base = groups[k] * size

        def body(s, _):
            visit(base + (mine_at + s) % size)
            return 0

        if short:
            for s in range(1 if k == 0 else 0, size):
                body(s, 0)
        else:
            lax.fori_loop(1 if k == 0 else 0, size, body, 0)

    def take(buf, sems, k):
        landed = buf.at[pl.ds(0, size - (1 if k == 0 else 0))]
        pltpu.make_async_copy(landed, landed, sems.at[k]).wait()

    for i in (RES, CHAIN, SINGLE):
        loads[i].start()
    barrier = pltpu.get_barrier_semaphore()
    for k in reversed(range(parts)):
        each_peer(k, lambda peer: pl.semaphore_signal(
            barrier, inc=1, device_id={"rows": peer}, device_id_type=pl.DeviceIdType.MESH))
    for i in (REL, WB, PAIR, COMPLEX, PAD, WQ, WG, WK, WV, WO, WMB, WMA, WHA, WHB, WHO, WP, PB):
        loads[i].start()

    arrive(RES, CHAIN)
    for k in range(0, count, step):
        code = chain_v[:, k:k + step].astype(f32) * chain_step + res_v[:, k:k + step].astype(f32)
        code_v[k:k + step, :] = jnp.broadcast_to(column(code), (step, 128))

    arrive(SINGLE)
    mine = single_v[...].astype(f32)
    normed = norm_rows(mine).astype(bf16)
    norm_s[...] = normed
    norm_r[me] = normed

    arrive(REL, WB, PAIR)
    rel = rel_v[...]
    tile_h = jnp.where(
        lax.broadcasted_iota(jnp.int32, (heads, spots), 1) % heads
        == lax.broadcasted_iota(jnp.int32, (heads, spots), 0), 1.0, 0.0).astype(bf16)
    w_tiled = mm_tn(wb_v[...], tile_h).astype(bf16)
    code_keys = code_v[pl.ds(first, rows), :classes]

    def bias_block(j, _):
        at = pl.multiple_of(j * step, step)
        code_i = code_v[pl.ds(at, step), :classes]
        diff = code_i[:, None, :] - code_keys[None, :, :]
        hot = bucket_onehot(diff.reshape(step * rows, classes), classes)
        cells = mm(hot, rel) + pair_v[pl.ds(at, step)].astype(f32).reshape(step * rows, width)
        out = mm(norm_rows(cells).astype(bf16), w_tiled)
        out = out.reshape(step // rows, rows, rows, spots)
        lane_q = lax.broadcasted_iota(jnp.int32, (1, 1, spots), 2) // heads
        total = jnp.where(lane_q == 0, out[:, 0], 0.0)
        for q in range(1, rows):
            total = jnp.where(lane_q == q, out[:, q], total)
        bias_s[pl.ds(pl.multiple_of(j * (step // rows), step // rows), step // rows)] = total.astype(bf16)
        return 0

    lax.fori_loop(0, count // step, bias_block, 0, unroll=short)
    bias_r[me] = bias_s[me]

    pl.semaphore_wait(barrier, n - 1)

    def remote(src, dst, i, k, peer):
        pltpu.make_async_remote_copy(
            src_ref=src, dst_ref=dst, send_sem=send_sem.at[i], recv_sem=recv_sem.at[i, k],
            device_id={"rows": peer}, device_id_type=pl.DeviceIdType.MESH).start()

    for k in reversed(range(parts)):
        each_peer(k, lambda peer: remote(norm_s, norm_r.at[me], 0, k, peer))
    for k in reversed(range(parts)):
        each_peer(k, lambda peer: remote(bias_s.at[peer], bias_r.at[me], 1, k, peer))

    def send_pair(k):
        each_peer(k, lambda peer: remote(
            pair_v.at[pl.ds(peer * rows, rows)], pair_r.at[me], 2, k, peer))

    arrive(WQ)
    queries = mm(normed, wq_v[...]).astype(bf16).astype(f32)
    arrive(WG)
    gating = jax.nn.sigmoid(mm(normed, wg_v[...]))
    head_of = lax.broadcasted_iota(jnp.int32, (heads, inner), 1) // head_size
    own_head = head_of == lax.broadcasted_iota(jnp.int32, (heads, inner), 0)
    q_wide = jnp.concatenate(
        [jnp.where(own_head, queries[q:q + 1, :], 0.0) for q in range(rows)], axis=0).astype(bf16)
    arrive(WK)
    toward = (mm_nt(wk_v[...], q_wide) / math.sqrt(head_size)).astype(bf16)

    arrive(COMPLEX, PAD)
    lane_spot = lax.broadcasted_iota(jnp.int32, (step, spots), 1) // heads
    for k in range(0, count, step):
        ccol_v[k:k + step, :] = jnp.broadcast_to(
            column(complex_v[:, k:k + step].astype(f32)), (step, 128))
    mine_c = ccol_v[pl.ds(first, rows), 0:1]
    lane_row = lax.broadcasted_iota(jnp.int32, (rows, spots), 1) // heads
    pick = lane_row == lax.broadcasted_iota(jnp.int32, (rows, spots), 0)
    query_c = jnp.sum(jnp.where(pick, mine_c, 0.0), axis=0, keepdims=True)
    for k in range(0, count, step):
        real = column(pad_v[:, k:k + step].astype(f32)) == 1.0
        same = ccol_v[k:k + step, :spots] == query_c
        itself = (lax.broadcasted_iota(jnp.int32, (step, spots), 0) + k) == (first + lane_spot)
        mask_v[k:k + step, :] = jnp.where(same & (real | itself), 0.0, masked_score)

    def rel_block(q, _):
        diff = code_v[pl.ds(first + q, 1), :classes] - code_v[:, :classes]
        pin_v[q] = mm(bucket_onehot(diff, classes), rel)
        return 0

    lax.fori_loop(0, rows, rel_block, 0, unroll=short)

    arrive(WHA, WHB, WHO, WP, PB)
    wha_v[...] = (wha_v[...].astype(f32) * 0.5).astype(bf16)
    bins = wp_v.shape[0]
    bias_col = column(pb_v[...])
    centers = (lax.broadcasted_iota(jnp.int32, (bins, 1), 0).astype(f32) + 0.5) * (32.0 / bins)
    arrive(WV, WO, WMB, WMA)

    pair_r[me] = pair_v[pl.ds(first, rows)]

    for k in range(parts):
        take(norm_r, recv_sem.at[0], k)
        if k == min(TRIGGER, parts - 1):
            for j in EARLY:
                send_pair(j)
    every = norm_r[...].astype(f32).reshape(count, inner).astype(bf16)
    scores = mm(every, toward)
    values = mm(every, wv_v[...]).astype(bf16)
    for k in range(parts):
        take(bias_r, recv_sem.at[1], k)
    scores = scores + bias_r[...].astype(f32).reshape(count, spots) + mask_v[...]
    expo = jnp.exp(scores - jnp.max(scores, axis=0, keepdims=True))
    weights = (expo * (1.0 / jnp.sum(expo, axis=0, keepdims=True))).astype(bf16)
    mixed_heads = mm_tn(weights, values)
    attended = jnp.concatenate(
        [jnp.sum(jnp.where(own_head, mixed_heads[q * heads:(q + 1) * heads, :], 0.0),
                 axis=0, keepdims=True) for q in range(rows)], axis=0)
    refined = (mine + mm((gating * attended).astype(bf16), wo_v[...])).astype(bf16)
    renormed = norm_rows(refined.astype(f32)).astype(bf16)
    factor_b = mm(renormed, wmb_v[...]).astype(bf16)
    b_s[...] = factor_b
    a_v[...] = mm(renormed, wma_v[...]).astype(bf16).astype(f32)
    b_r[me] = factor_b
    refined_ref[...] = refined

    for k in reversed(range(parts)):
        each_peer(k, lambda peer: remote(b_s, b_r.at[me], 3, k, peer))
    for k in LATE:
        send_pair(k)

    def tail(ks, off):
        spans = [pl.multiple_of(groups[k] * span + off, sub) for k in ks]
        total = len(ks) * rows * sub
        for i, at in enumerate(spans):
            near = pl.ds(at // rows, sub // rows)
            factor = b_r[near].astype(f32).reshape(sub, width)
            for q in range(rows):
                flat = (pin_v[q, pl.ds(at, sub), :] + pair_r[near, q].astype(f32).reshape(sub, width)
                        + a_v[q:q + 1, :] * factor)
                row = (i * rows + q) * sub
                flat_v[row:row + sub, :] = flat
                x_v[row:row + sub, :] = norm_rows(flat).astype(bf16)
        cut = 256
        tall = 128
        for k in range(0, wha_v.shape[1], cut):
            wa = wha_v[:, k:k + cut]
            wb = whb_v[:, k:k + cut]
            for r in range(0, total, tall):
                x = x_v[r:r + tall, :]
                half = mm(x, wa)
                up = mm(x, wb)
                hid_v[r:r + tall, k:k + cut] = ((half + half * jnp.tanh(half)) * up).astype(bf16)
        for r in range(0, total, tall):
            updated = flat_v[r:r + tall, :] + mm(hid_v[r:r + tall, :], who_v[...])
            x_v[r:r + tall, :] = norm_rows(updated).astype(bf16)
        per = tall // sub
        lane_part = lax.broadcasted_iota(jnp.int32, (rows, tall), 1) // sub
        row_part = lax.broadcasted_iota(jnp.int32, (rows, tall), 0) % per
        row_block = lax.broadcasted_iota(jnp.int32, (rows, tall), 0) // per
        for i, at in enumerate(spans):
            found = jnp.zeros((rows, tall), f32)
            for v in range(rows // per):
                r = i * rows * sub + v * tall
                logits = mm_nt(wp_v[...], x_v[r:r + tall, :]) + bias_col
                expo = jnp.exp(logits - jnp.max(logits, axis=0, keepdims=True))
                value = (jnp.sum(expo * centers, axis=0, keepdims=True)
                         / jnp.sum(expo, axis=0, keepdims=True))
                found = jnp.where(row_block == v, value, found)
            spread = found
            for u in range(1, per):
                spread = jnp.where((lane_part + per - row_part) % per == u,
                                   pltpu.roll(found, u * sub, 1), spread)
            where = pl.ds(pl.multiple_of(at // tall * tall, tall), tall)
            errors_ref[:, where] = jnp.where(
                lane_part == (at // sub) % per, spread, errors_ref[:, where])

    errors_ref[...] = jnp.zeros_like(errors_ref)
    for name, ks in PIECES:
        for k in ks:
            take(pair_r, recv_sem.at[2], k)
        for k in ks:
            take(b_r, recv_sem.at[3], k)
        if short:
            tail(ks, 0)
        else:
            def more(c, _):
                tail(ks, c * sub)
                return 0

            lax.fori_loop(0, span // sub, more, 0)

    for i, buf in enumerate((norm_r, bias_r, pair_r, b_r)):
        sent = buf.at[pl.ds(0, n - 1)]
        pltpu.make_async_copy(sent, sent, send_sem.at[i]).wait()


def place(refined_v, errors_v, refined_h, errors_h, sem):
    copies = (
        pltpu.make_async_copy(refined_v, refined_h, sem.at[0]),
        pltpu.make_async_copy(errors_v, errors_h, sem.at[1]),
    )
    for copy in copies:
        copy.start()
    for copy in copies:
        copy.wait()


def on_device(n, pair_repr, single_repr, residue_index, chain_index, complex_index, pad_mask,
              w_query, w_key, w_value, w_gate, w_out, w_bias, rel_table, w_mix_a, w_mix_b,
              w_hidden_a, w_hidden_b, w_hidden_out, w_pae, pae_bias):
    count, rows, width = pair_repr.shape
    inner = single_repr.shape[1]
    heads = w_bias.shape[1]
    hidden = w_hidden_a.shape[1]
    args = (pair_repr, single_repr, residue_index[None], chain_index[None], complex_index[None],
            pad_mask[None], w_query, w_key, w_value, w_gate, w_out, w_bias.T, rel_table,
            w_mix_a, w_mix_b, w_hidden_a, w_hidden_b, w_hidden_out, w_pae.T, pae_bias[None])
    spots = rows * heads
    step = min(count, 128)
    scratch = [pltpu.VMEM(a.shape, a.dtype) for a in args] + [
        pltpu.VMEM((count, 128), f32),
        pltpu.VMEM((count, 128), f32),
        pltpu.VMEM((count, spots), f32),
        pltpu.VMEM((n, rows, spots), bf16),
        pltpu.VMEM((n, rows, spots), bf16),
        pltpu.VMEM((rows, inner), bf16),
        pltpu.VMEM((n, rows, inner), bf16),
        pltpu.VMEM((n, rows, rows, width), bf16),
        pltpu.VMEM((rows, width), bf16),
        pltpu.VMEM((n, rows, width), bf16),
        pltpu.VMEM((rows, width), f32),
        pltpu.VMEM((rows, count, width), f32),
        pltpu.VMEM((rows * step, width), f32),
        pltpu.VMEM((rows * step, width), bf16),
        pltpu.VMEM((rows * step, hidden), bf16),
        pltpu.SemaphoreType.DMA((len(args),)),
        pltpu.SemaphoreType.DMA((4,)),
        pltpu.SemaphoreType.DMA((4, 4)),
    ]
    refined, errors = pl.pallas_call(
        functools.partial(kernel, n, heads),
        out_shape=(pltpu.VMEM((rows, inner), bf16), pltpu.VMEM((rows, count), f32)),
        in_specs=[pl.BlockSpec(memory_space=pltpu.HBM)] * len(args),
        out_specs=[pl.BlockSpec(memory_space=pltpu.VMEM)] * 2,
        scratch_shapes=scratch,
        compiler_params=pltpu.CompilerParams(
            collective_id=0, has_side_effects=True, vmem_limit_bytes=40 * 1024 * 1024),
        name="confidence",
    )(*[pltpu.with_memory_space_constraint(a, pltpu.HBM) for a in args])
    return pl.pallas_call(
        place,
        out_shape=(
            jax.ShapeDtypeStruct((rows, inner), bf16),
            jax.ShapeDtypeStruct((rows, count), f32),
        ),
        in_specs=[pl.BlockSpec(memory_space=pltpu.VMEM)] * 2,
        out_specs=[pl.BlockSpec(memory_space=pltpu.HBM)] * 2,
        scratch_shapes=[pltpu.SemaphoreType.DMA((2,))],
        compiler_params=pltpu.CompilerParams(vmem_limit_bytes=1024 * 1024),
        name="place",
    )(refined, errors)


def solution(mesh):
    placed = (
        P("groups", "rows", None),
        P(("groups", "rows"), None),
        P("groups"),
        P("groups"),
        P("groups"),
        P("groups"),
    ) + (P(),) * 14
    return jax.shard_map(
        functools.partial(on_device, mesh.shape["rows"]),
        mesh=mesh,
        in_specs=placed,
        out_specs=(P(("groups", "rows"), None), P(("groups", "rows"), None)),
        check_vma=False,
    )
```

```python
import functools
import math

import jax
import jax.numpy as jnp
from jax import lax
from jax.experimental import pallas as pl
from jax.experimental.pallas import tpu as pltpu
from jax.sharding import PartitionSpec as P

epsilon = 1e-05
masked_score = -1e30
chain_step = 65536.0
f32 = jnp.float32
bf16 = jnp.bfloat16


EARLY = (2, 1, 0)
LATE = (3,)
TRIGGER = 0
PIECES = (("a", (0, 1)), ("b", (2, 3)))


def norm_rows(values):
    center = values - jnp.mean(values, axis=-1, keepdims=True)
    spread = jnp.mean(center * center, axis=-1, keepdims=True)
    return center * lax.rsqrt(spread + epsilon)


def mm(a, b):
    return jnp.dot(a, b, preferred_element_type=f32)


def mm_nt(a, b):
    return lax.dot_general(a, b, (((1,), (1,)), ((), ())), preferred_element_type=f32)


def mm_tn(a, b):
    return lax.dot_general(a, b, (((0,), (0,)), ((), ())), preferred_element_type=f32)


def column(row):
    m = row.shape[1]
    pick = lax.broadcasted_iota(jnp.int32, (m, m), 0) == lax.broadcasted_iota(jnp.int32, (m, m), 1)
    return jnp.sum(jnp.where(pick, row, 0.0), axis=1, keepdims=True)


def bucket_onehot(diff, classes):
    reach = (classes - 2) // 2
    same = jnp.abs(diff) < 0.5 * chain_step
    bucket = jnp.where(same, jnp.clip(diff, -reach, reach) + reach, 2.0 * reach + 1.0)
    lanes = lax.broadcasted_iota(jnp.int32, bucket.shape, bucket.ndim - 1).astype(f32)
    return jnp.where(bucket == lanes, 1.0, 0.0).astype(bf16)


def kernel(
    n,
    heads,
    pair_h, single_h, res_h, chain_h, complex_h, pad_h,
    wq_h, wk_h, wv_h, wg_h, wo_h, wb_h, rel_h, wma_h, wmb_h, wha_h, whb_h, who_h, wp_h, pb_h,
    refined_ref, errors_ref,
    pair_v, single_v, res_v, chain_v, complex_v, pad_v,
    wq_v, wk_v, wv_v, wg_v, wo_v, wb_v, rel_v, wma_v, wmb_v, wha_v, whb_v, who_v, wp_v, pb_v,
    code_v, ccol_v, mask_v, bias_s, bias_r, norm_s, norm_r, pair_r, b_s, b_r, a_v, pin_v,
    flat_v, x_v, hid_v,
    local_sem, send_sem, recv_sem,
):
    me = lax.axis_index("rows")
    count, rows, width = pair_h.shape
    classes = rel_h.shape[0]
    inner = single_h.shape[1]
    head_size = inner // heads
    spots = rows * heads
    first = pl.multiple_of(me * rows, rows)
    step = min(count, 128)
    short = count == step
    sub = 32

    hbm = (pair_h, single_h, res_h, chain_h, complex_h, pad_h, wq_h, wk_h, wv_h, wg_h, wo_h,
           wb_h, rel_h, wma_h, wmb_h, wha_h, whb_h, who_h, wp_h, pb_h)
    vmem = (pair_v, single_v, res_v, chain_v, complex_v, pad_v, wq_v, wk_v, wv_v, wg_v, wo_v,
            wb_v, rel_v, wma_v, wmb_v, wha_v, whb_v, who_v, wp_v, pb_v)
    (PAIR, SINGLE, RES, CHAIN, COMPLEX, PAD, WQ, WK, WV, WG, WO, WB, REL, WMA, WMB, WHA, WHB,
     WHO, WP, PB) = range(len(hbm))
    loads = [pltpu.make_async_copy(h, v, local_sem.at[i]) for i, (h, v) in enumerate(zip(hbm, vmem))]

    def arrive(*which):
        for i in which:
            loads[i].wait()

    parts = 4 if n % 4 == 0 else 1
    size = n // parts
    mine_at = me % size
    group = me // size
    low = group % 2
    groups = (group, group + 1 - 2 * low, group + 2 - 4 * (group // 2), 3 - group)[:parts]
    span = size * rows

    def each_peer(k, visit):
        base = groups[k] * size

        def body(s, _):
            visit(base + (mine_at + s) % size)
            return 0

        if short:
            for s in range(1 if k == 0 else 0, size):
                body(s, 0)
        else:
            lax.fori_loop(1 if k == 0 else 0, size, body, 0)

    def take(buf, sems, k):
        landed = buf.at[pl.ds(0, size - (1 if k == 0 else 0))]
        pltpu.make_async_copy(landed, landed, sems.at[k]).wait()

    for i in (RES, CHAIN, SINGLE):
        loads[i].start()
    barrier = pltpu.get_barrier_semaphore()
    for k in reversed(range(parts)):
        each_peer(k, lambda peer: pl.semaphore_signal(
            barrier, inc=1, device_id={"rows": peer}, device_id_type=pl.DeviceIdType.MESH))
    for i in (REL, WB, PAIR, COMPLEX, PAD, WQ, WG, WK, WV, WO, WMB, WMA, WHA, WHB, WHO, WP, PB):
        loads[i].start()

    arrive(RES, CHAIN)
    for k in range(0, count, step):
        code = chain_v[:, k:k + step].astype(f32) * chain_step + res_v[:, k:k + step].astype(f32)
        code_v[k:k + step, :] = jnp.broadcast_to(column(code), (step, 128))

    arrive(SINGLE)
    mine = single_v[...].astype(f32)
    normed = norm_rows(mine).astype(bf16)
    norm_s[...] = normed
    norm_r[me] = normed

    arrive(REL, WB, PAIR)
    rel = rel_v[...]
    tile_h = jnp.where(
        lax.broadcasted_iota(jnp.int32, (heads, spots), 1) % heads
        == lax.broadcasted_iota(jnp.int32, (heads, spots), 0), 1.0, 0.0).astype(bf16)
    w_tiled = mm_tn(wb_v[...], tile_h).astype(bf16)
    code_keys = code_v[pl.ds(first, rows), :classes]

    def bias_block(j, _):
        at = pl.multiple_of(j * step, step)
        code_i = code_v[pl.ds(at, step), :classes]
        diff = code_i[:, None, :] - code_keys[None, :, :]
        hot = bucket_onehot(diff.reshape(step * rows, classes), classes)
        cells = mm(hot, rel) + pair_v[pl.ds(at, step)].astype(f32).reshape(step * rows, width)
        out = mm(norm_rows(cells).astype(bf16), w_tiled)
        out = out.reshape(step // rows, rows, rows, spots)
        lane_q = lax.broadcasted_iota(jnp.int32, (1, 1, spots), 2) // heads
        total = jnp.where(lane_q == 0, out[:, 0], 0.0)
        for q in range(1, rows):
            total = jnp.where(lane_q == q, out[:, q], total)
        bias_s[pl.ds(pl.multiple_of(j * (step // rows), step // rows), step // rows)] = total.astype(bf16)
        return 0

    lax.fori_loop(0, count // step, bias_block, 0, unroll=short)
    bias_r[me] = bias_s[me]

    pl.semaphore_wait(barrier, n - 1)

    def remote(src, dst, i, k, peer):
        pltpu.make_async_remote_copy(
            src_ref=src, dst_ref=dst, send_sem=send_sem.at[i], recv_sem=recv_sem.at[i, k],
            device_id={"rows": peer}, device_id_type=pl.DeviceIdType.MESH).start()

    for k in reversed(range(parts)):
        each_peer(k, lambda peer: remote(norm_s, norm_r.at[me], 0, k, peer))
    for k in reversed(range(parts)):
        each_peer(k, lambda peer: remote(bias_s.at[peer], bias_r.at[me], 1, k, peer))

    def send_pair(k):
        each_peer(k, lambda peer: remote(
            pair_v.at[pl.ds(peer * rows, rows)], pair_r.at[me], 2, k, peer))

    def send_pair_either(edge, middle):
        inside = group * (3 - group) // 2
        k = edge + (middle - edge) * inside
        base = (groups[edge] + (groups[middle] - groups[edge]) * inside) * size
        for s in range(size) if short else ():
            peer = base + (mine_at + s) % size
            remote(pair_v.at[pl.ds(peer * rows, rows)], pair_r.at[me], 2, k, peer)
        if not short:
            def body(s, _):
                peer = base + (mine_at + s) % size
                remote(pair_v.at[pl.ds(peer * rows, rows)], pair_r.at[me], 2, k, peer)
                return 0

            lax.fori_loop(0, size, body, 0)

    arrive(WQ)
    queries = mm(normed, wq_v[...]).astype(bf16).astype(f32)
    arrive(WG)
    gating = jax.nn.sigmoid(mm(normed, wg_v[...]))
    head_of = lax.broadcasted_iota(jnp.int32, (heads, inner), 1) // head_size
    own_head = head_of == lax.broadcasted_iota(jnp.int32, (heads, inner), 0)
    q_wide = jnp.concatenate(
        [jnp.where(own_head, queries[q:q + 1, :], 0.0) for q in range(rows)], axis=0).astype(bf16)
    arrive(WK)
    toward = (mm_nt(wk_v[...], q_wide) / math.sqrt(head_size)).astype(bf16)

    arrive(COMPLEX, PAD)
    lane_spot = lax.broadcasted_iota(jnp.int32, (step, spots), 1) // heads
    for k in range(0, count, step):
        ccol_v[k:k + step, :] = jnp.broadcast_to(
            column(complex_v[:, k:k + step].astype(f32)), (step, 128))
    mine_c = ccol_v[pl.ds(first, rows), 0:1]
    lane_row = lax.broadcasted_iota(jnp.int32, (rows, spots), 1) // heads
    pick = lane_row == lax.broadcasted_iota(jnp.int32, (rows, spots), 0)
    query_c = jnp.sum(jnp.where(pick, mine_c, 0.0), axis=0, keepdims=True)
    for k in range(0, count, step):
        real = column(pad_v[:, k:k + step].astype(f32)) == 1.0
        same = ccol_v[k:k + step, :spots] == query_c
        itself = (lax.broadcasted_iota(jnp.int32, (step, spots), 0) + k) == (first + lane_spot)
        mask_v[k:k + step, :] = jnp.where(same & (real | itself), 0.0, masked_score)

    def rel_block(q, _):
        diff = code_v[pl.ds(first + q, 1), :classes] - code_v[:, :classes]
        pin_v[q] = mm(bucket_onehot(diff, classes), rel)
        return 0

    lax.fori_loop(0, rows, rel_block, 0, unroll=short)

    arrive(WHA, WHB, WHO, WP, PB)
    wha_v[...] = (wha_v[...].astype(f32) * 0.5).astype(bf16)
    bins = wp_v.shape[0]
    bias_col = column(pb_v[...])
    centers = (lax.broadcasted_iota(jnp.int32, (bins, 1), 0).astype(f32) + 0.5) * (32.0 / bins)
    arrive(WV, WO, WMB, WMA)

    pair_r[me] = pair_v[pl.ds(first, rows)]

    for k in range(parts):
        take(norm_r, recv_sem.at[0], k)
        if k == min(TRIGGER, parts - 1):
            send_pair_either(3, 2)
            send_pair(1)
            send_pair(0)
    every = norm_r[...].astype(f32).reshape(count, inner).astype(bf16)
    scores = mm(every, toward)
    values = mm(every, wv_v[...]).astype(bf16)
    for k in range(parts):
        take(bias_r, recv_sem.at[1], k)
    scores = scores + bias_r[...].astype(f32).reshape(count, spots) + mask_v[...]
    expo = jnp.exp(scores - jnp.max(scores, axis=0, keepdims=True))
    weights = (expo * (1.0 / jnp.sum(expo, axis=0, keepdims=True))).astype(bf16)
    mixed_heads = mm_tn(weights, values)
    attended = jnp.concatenate(
        [jnp.sum(jnp.where(own_head, mixed_heads[q * heads:(q + 1) * heads, :], 0.0),
                 axis=0, keepdims=True) for q in range(rows)], axis=0)
    refined = (mine + mm((gating * attended).astype(bf16), wo_v[...])).astype(bf16)
    renormed = norm_rows(refined.astype(f32)).astype(bf16)
    factor_b = mm(renormed, wmb_v[...]).astype(bf16)
    b_s[...] = factor_b
    a_v[...] = mm(renormed, wma_v[...]).astype(bf16).astype(f32)
    b_r[me] = factor_b
    refined_ref[...] = refined

    for k in reversed(range(parts)):
        each_peer(k, lambda peer: remote(b_s, b_r.at[me], 3, k, peer))
    send_pair_either(2, 3)

    def tail(ks, off):
        spans = [pl.multiple_of(groups[k] * span + off, sub) for k in ks]
        total = len(ks) * rows * sub
        for i, at in enumerate(spans):
            near = pl.ds(at // rows, sub // rows)
            factor = b_r[near].astype(f32).reshape(sub, width)
            for q in range(rows):
                flat = (pin_v[q, pl.ds(at, sub), :] + pair_r[near, q].astype(f32).reshape(sub, width)
                        + a_v[q:q + 1, :] * factor)
                row = (i * rows + q) * sub
                flat_v[row:row + sub, :] = flat
                x_v[row:row + sub, :] = norm_rows(flat).astype(bf16)
        cut = 256
        tall = 128
        for k in range(0, wha_v.shape[1], cut):
            wa = wha_v[:, k:k + cut]
            wb = whb_v[:, k:k + cut]
            for r in range(0, total, tall):
                x = x_v[r:r + tall, :]
                half = mm(x, wa)
                up = mm(x, wb)
                hid_v[r:r + tall, k:k + cut] = ((half + half * jnp.tanh(half)) * up).astype(bf16)
        for r in range(0, total, tall):
            updated = flat_v[r:r + tall, :] + mm(hid_v[r:r + tall, :], who_v[...])
            x_v[r:r + tall, :] = norm_rows(updated).astype(bf16)
        per = tall // sub
        lane_part = lax.broadcasted_iota(jnp.int32, (rows, tall), 1) // sub
        row_part = lax.broadcasted_iota(jnp.int32, (rows, tall), 0) % per
        row_block = lax.broadcasted_iota(jnp.int32, (rows, tall), 0) // per
        for i, at in enumerate(spans):
            found = jnp.zeros((rows, tall), f32)
            for v in range(rows // per):
                r = i * rows * sub + v * tall
                logits = mm_nt(wp_v[...], x_v[r:r + tall, :]) + bias_col
                expo = jnp.exp(logits - jnp.max(logits, axis=0, keepdims=True))
                value = (jnp.sum(expo * centers, axis=0, keepdims=True)
                         / jnp.sum(expo, axis=0, keepdims=True))
                found = jnp.where(row_block == v, value, found)
            spread = found
            for u in range(1, per):
                spread = jnp.where((lane_part + per - row_part) % per == u,
                                   pltpu.roll(found, u * sub, 1), spread)
            where = pl.ds(pl.multiple_of(at // tall * tall, tall), tall)
            errors_ref[:, where] = jnp.where(
                lane_part == (at // sub) % per, spread, errors_ref[:, where])

    errors_ref[...] = jnp.zeros_like(errors_ref)
    for name, ks in PIECES:
        for k in ks:
            take(pair_r, recv_sem.at[2], k)
        for k in ks:
            take(b_r, recv_sem.at[3], k)
        if short:
            tail(ks, 0)
        else:
            def more(c, _):
                tail(ks, c * sub)
                return 0

            lax.fori_loop(0, span // sub, more, 0)

    for i, buf in enumerate((norm_r, bias_r, pair_r, b_r)):
        sent = buf.at[pl.ds(0, n - 1)]
        pltpu.make_async_copy(sent, sent, send_sem.at[i]).wait()


def place(refined_v, errors_v, refined_h, errors_h, sem):
    copies = (
        pltpu.make_async_copy(refined_v, refined_h, sem.at[0]),
        pltpu.make_async_copy(errors_v, errors_h, sem.at[1]),
    )
    for copy in copies:
        copy.start()
    for copy in copies:
        copy.wait()


def on_device(n, pair_repr, single_repr, residue_index, chain_index, complex_index, pad_mask,
              w_query, w_key, w_value, w_gate, w_out, w_bias, rel_table, w_mix_a, w_mix_b,
              w_hidden_a, w_hidden_b, w_hidden_out, w_pae, pae_bias):
    count, rows, width = pair_repr.shape
    inner = single_repr.shape[1]
    heads = w_bias.shape[1]
    hidden = w_hidden_a.shape[1]
    args = (pair_repr, single_repr, residue_index[None], chain_index[None], complex_index[None],
            pad_mask[None], w_query, w_key, w_value, w_gate, w_out, w_bias.T, rel_table,
            w_mix_a, w_mix_b, w_hidden_a, w_hidden_b, w_hidden_out, w_pae.T, pae_bias[None])
    spots = rows * heads
    step = min(count, 128)
    scratch = [pltpu.VMEM(a.shape, a.dtype) for a in args] + [
        pltpu.VMEM((count, 128), f32),
        pltpu.VMEM((count, 128), f32),
        pltpu.VMEM((count, spots), f32),
        pltpu.VMEM((n, rows, spots), bf16),
        pltpu.VMEM((n, rows, spots), bf16),
        pltpu.VMEM((rows, inner), bf16),
        pltpu.VMEM((n, rows, inner), bf16),
        pltpu.VMEM((n, rows, rows, width), bf16),
        pltpu.VMEM((rows, width), bf16),
        pltpu.VMEM((n, rows, width), bf16),
        pltpu.VMEM((rows, width), f32),
        pltpu.VMEM((rows, count, width), f32),
        pltpu.VMEM((rows * step, width), f32),
        pltpu.VMEM((rows * step, width), bf16),
        pltpu.VMEM((rows * step, hidden), bf16),
        pltpu.SemaphoreType.DMA((len(args),)),
        pltpu.SemaphoreType.DMA((4,)),
        pltpu.SemaphoreType.DMA((4, 4)),
    ]
    refined, errors = pl.pallas_call(
        functools.partial(kernel, n, heads),
        out_shape=(pltpu.VMEM((rows, inner), bf16), pltpu.VMEM((rows, count), f32)),
        in_specs=[pl.BlockSpec(memory_space=pltpu.HBM)] * len(args),
        out_specs=[pl.BlockSpec(memory_space=pltpu.VMEM)] * 2,
        scratch_shapes=scratch,
        compiler_params=pltpu.CompilerParams(
            collective_id=0, has_side_effects=True, vmem_limit_bytes=40 * 1024 * 1024),
        name="confidence",
    )(*[pltpu.with_memory_space_constraint(a, pltpu.HBM) for a in args])
    return pl.pallas_call(
        place,
        out_shape=(
            jax.ShapeDtypeStruct((rows, inner), bf16),
            jax.ShapeDtypeStruct((rows, count), f32),
        ),
        in_specs=[pl.BlockSpec(memory_space=pltpu.VMEM)] * 2,
        out_specs=[pl.BlockSpec(memory_space=pltpu.HBM)] * 2,
        scratch_shapes=[pltpu.SemaphoreType.DMA((2,))],
        compiler_params=pltpu.CompilerParams(vmem_limit_bytes=1024 * 1024),
        name="place",
    )(refined, errors)


def solution(mesh):
    placed = (
        P("groups", "rows", None),
        P(("groups", "rows"), None),
        P("groups"),
        P("groups"),
        P("groups"),
        P("groups"),
    ) + (P(),) * 14
    return jax.shard_map(
        functools.partial(on_device, mesh.shape["rows"]),
        mesh=mesh,
        in_specs=placed,
        out_specs=(P(("groups", "rows"), None), P(("groups", "rows"), None)),
        check_vma=False,
    )
```

```python
import functools
import math

import jax
import jax.numpy as jnp
from jax import lax
from jax.experimental import pallas as pl
from jax.experimental.pallas import tpu as pltpu
from jax.sharding import PartitionSpec as P

epsilon = 1e-05
masked_score = -1e30
chain_step = 65536.0
f32 = jnp.float32
bf16 = jnp.bfloat16


TRIGGER = 0


def norm_rows(values):
    center = values - jnp.mean(values, axis=-1, keepdims=True)
    spread = jnp.mean(center * center, axis=-1, keepdims=True)
    return center * lax.rsqrt(spread + epsilon)


def mm(a, b):
    return jnp.dot(a, b, preferred_element_type=f32)


def mm_nt(a, b):
    return lax.dot_general(a, b, (((1,), (1,)), ((), ())), preferred_element_type=f32)


def mm_tn(a, b):
    return lax.dot_general(a, b, (((0,), (0,)), ((), ())), preferred_element_type=f32)


def column(row):
    m = row.shape[1]
    pick = lax.broadcasted_iota(jnp.int32, (m, m), 0) == lax.broadcasted_iota(jnp.int32, (m, m), 1)
    return jnp.sum(jnp.where(pick, row, 0.0), axis=1, keepdims=True)


def bucket_onehot(diff, classes):
    reach = (classes - 2) // 2
    same = jnp.abs(diff) < 0.5 * chain_step
    bucket = jnp.where(same, jnp.clip(diff, -reach, reach) + reach, 2.0 * reach + 1.0)
    lanes = lax.broadcasted_iota(jnp.int32, bucket.shape, bucket.ndim - 1).astype(f32)
    return jnp.where(bucket == lanes, 1.0, 0.0).astype(bf16)


def kernel(
    n,
    heads,
    pair_h, single_h, res_h, chain_h, complex_h, pad_h,
    wq_h, wk_h, wv_h, wg_h, wo_h, wb_h, rel_h, wma_h, wmb_h, wha_h, whb_h, who_h, wp_h, pb_h,
    refined_ref, errors_ref,
    pair_v, single_v, res_v, chain_v, complex_v, pad_v,
    wq_v, wk_v, wv_v, wg_v, wo_v, wb_v, rel_v, wma_v, wmb_v, wha_v, whb_v, who_v, wp_v, pb_v,
    code_v, ccol_v, mask_v, bias_s, bias_r, norm_s, norm_r, pair_r, b_s, b_r, a_v, pin_v,
    flat_v, x_v, hid_v, wab_v,
    local_sem, send_sem, recv_sem,
):
    me = lax.axis_index("rows")
    count, rows, width = pair_h.shape
    classes = rel_h.shape[0]
    inner = single_h.shape[1]
    head_size = inner // heads
    spots = rows * heads
    first = pl.multiple_of(me * rows, rows)
    step = min(count, 128)
    short = count == step
    sub = 32

    hbm = (pair_h, single_h, res_h, chain_h, complex_h, pad_h, wq_h, wk_h, wv_h, wg_h, wo_h,
           wb_h, rel_h, wma_h, wmb_h, wha_h, whb_h, who_h, wp_h, pb_h)
    vmem = (pair_v, single_v, res_v, chain_v, complex_v, pad_v, wq_v, wk_v, wv_v, wg_v, wo_v,
            wb_v, rel_v, wma_v, wmb_v, wha_v, whb_v, who_v, wp_v, pb_v)
    (PAIR, SINGLE, RES, CHAIN, COMPLEX, PAD, WQ, WK, WV, WG, WO, WB, REL, WMA, WMB, WHA, WHB,
     WHO, WP, PB) = range(len(hbm))
    loads = [pltpu.make_async_copy(h, v, local_sem.at[i]) for i, (h, v) in enumerate(zip(hbm, vmem))]

    def arrive(*which):
        for i in which:
            loads[i].wait()

    parts = 4 if n % 4 == 0 else 1
    size = n // parts
    mine_at = me % size
    group = me // size
    low = group % 2
    groups = (group, group + 1 - 2 * low, group + 2 - 4 * (group // 2), 3 - group)[:parts]
    span = size * rows

    def each_peer(k, visit):
        base = groups[k] * size

        def body(s, _):
            visit(base + (mine_at + s) % size)
            return 0

        if short:
            for s in range(1 if k == 0 else 0, size):
                body(s, 0)
        else:
            lax.fori_loop(1 if k == 0 else 0, size, body, 0)

    def take(buf, sems, k):
        landed = buf.at[pl.ds(0, size - (1 if k == 0 else 0))]
        pltpu.make_async_copy(landed, landed, sems.at[k]).wait()

    for i in (RES, CHAIN, SINGLE):
        loads[i].start()
    barrier = pltpu.get_barrier_semaphore()
    for k in reversed(range(parts)):
        each_peer(k, lambda peer: pl.semaphore_signal(
            barrier, inc=1, device_id={"rows": peer}, device_id_type=pl.DeviceIdType.MESH))
    for i in (REL, WB, PAIR, COMPLEX, PAD, WQ, WG, WK, WV, WO, WMB, WMA, WHA, WHB, WHO, WP, PB):
        loads[i].start()

    arrive(RES, CHAIN)
    for k in range(0, count, step):
        code = chain_v[:, k:k + step].astype(f32) * chain_step + res_v[:, k:k + step].astype(f32)
        code_v[k:k + step, :] = jnp.broadcast_to(column(code), (step, 128))

    arrive(SINGLE)
    mine = single_v[...].astype(f32)
    normed = norm_rows(mine).astype(bf16)
    norm_s[...] = normed
    norm_r[me // 2, me % 2] = normed

    arrive(REL, WB, PAIR)
    rel = rel_v[...]
    tile_h = jnp.where(
        lax.broadcasted_iota(jnp.int32, (heads, spots), 1) % heads
        == lax.broadcasted_iota(jnp.int32, (heads, spots), 0), 1.0, 0.0).astype(bf16)
    w_tiled = mm_tn(wb_v[...], tile_h).astype(bf16)
    code_keys = code_v[pl.ds(first, rows), :classes]

    def bias_block(j, _):
        at = pl.multiple_of(j * step, step)
        code_i = code_v[pl.ds(at, step), :classes]
        diff = code_i[:, None, :] - code_keys[None, :, :]
        hot = bucket_onehot(diff.reshape(step * rows, classes), classes)
        cells = mm(hot, rel) + pair_v[pl.ds(at, step)].astype(f32).reshape(step * rows, width)
        out = mm(norm_rows(cells).astype(bf16), w_tiled)
        out = out.reshape(step // rows, rows, rows, spots)
        lane_q = lax.broadcasted_iota(jnp.int32, (1, 1, spots), 2) // heads
        total = jnp.where(lane_q == 0, out[:, 0], 0.0)
        for q in range(1, rows):
            total = jnp.where(lane_q == q, out[:, q], total)
        bias_s[pl.ds(pl.multiple_of(j * (step // rows), step // rows), step // rows)] = total.astype(bf16)
        return 0

    lax.fori_loop(0, count // step, bias_block, 0, unroll=short)
    bias_r[me] = bias_s[me]

    pl.semaphore_wait(barrier, n - 1)

    def remote(src, dst, i, k, peer):
        pltpu.make_async_remote_copy(
            src_ref=src, dst_ref=dst, send_sem=send_sem.at[i], recv_sem=recv_sem.at[i, k],
            device_id={"rows": peer}, device_id_type=pl.DeviceIdType.MESH).start()

    side = me % 2
    partner = me + 1 - 2 * side
    pairs = size // 2

    def spread_single(k):
        base = groups[k] * size

        def body(s, _):
            chip = base + 2 * ((mine_at // 2 + s) % pairs)
            for core in (0, 1) if k == 0 else (side,):
                remote(norm_s, norm_r.at[me // 2, side], 0, k, chip + core)
            return 0

        if short:
            for s in range(1 if k == 0 else 0, pairs):
                body(s, 0)
        else:
            lax.fori_loop(1 if k == 0 else 0, pairs, body, 0)
        if k == 0:
            remote(norm_s, norm_r.at[me // 2, side], 5, 0, partner)

    for k in reversed(range(parts)):
        spread_single(k)
    for k in reversed(range(parts)):
        each_peer(k, lambda peer: remote(bias_s.at[peer], bias_r.at[me], 1, k, peer))

    def send_pair(k):
        each_peer(k, lambda peer: remote(
            pair_v.at[pl.ds(peer * rows, rows)], pair_r.at[me], 2, k, peer))

    def send_pair_either(edge, middle):
        inside = group * (3 - group) // 2
        k = edge + (middle - edge) * inside
        base = (groups[edge] + (groups[middle] - groups[edge]) * inside) * size
        for s in range(size) if short else ():
            peer = base + (mine_at + s) % size
            remote(pair_v.at[pl.ds(peer * rows, rows)], pair_r.at[me], 2, k, peer)
        if not short:
            def body(s, _):
                peer = base + (mine_at + s) % size
                remote(pair_v.at[pl.ds(peer * rows, rows)], pair_r.at[me], 2, k, peer)
                return 0

            lax.fori_loop(0, size, body, 0)

    arrive(WQ)
    queries = mm(normed, wq_v[...]).astype(bf16).astype(f32)
    arrive(WG)
    gating = jax.nn.sigmoid(mm(normed, wg_v[...]))
    head_of = lax.broadcasted_iota(jnp.int32, (heads, inner), 1) // head_size
    own_head = head_of == lax.broadcasted_iota(jnp.int32, (heads, inner), 0)
    q_wide = jnp.concatenate(
        [jnp.where(own_head, queries[q:q + 1, :], 0.0) for q in range(rows)], axis=0).astype(bf16)
    arrive(WK)
    toward = (mm_nt(wk_v[...], q_wide) / math.sqrt(head_size)).astype(bf16)

    arrive(COMPLEX, PAD)
    lane_spot = lax.broadcasted_iota(jnp.int32, (step, spots), 1) // heads
    for k in range(0, count, step):
        ccol_v[k:k + step, :] = jnp.broadcast_to(
            column(complex_v[:, k:k + step].astype(f32)), (step, 128))
    mine_c = ccol_v[pl.ds(first, rows), 0:1]
    lane_row = lax.broadcasted_iota(jnp.int32, (rows, spots), 1) // heads
    pick = lane_row == lax.broadcasted_iota(jnp.int32, (rows, spots), 0)
    query_c = jnp.sum(jnp.where(pick, mine_c, 0.0), axis=0, keepdims=True)
    for k in range(0, count, step):
        real = column(pad_v[:, k:k + step].astype(f32)) == 1.0
        same = ccol_v[k:k + step, :spots] == query_c
        itself = (lax.broadcasted_iota(jnp.int32, (step, spots), 0) + k) == (first + lane_spot)
        mask_v[k:k + step, :] = jnp.where(same & (real | itself), 0.0, masked_score)

    def rel_block(q, _):
        diff = code_v[pl.ds(first + q, 1), :classes] - code_v[:, :classes]
        pin_v[q] = mm(bucket_onehot(diff, classes), rel)
        return 0

    lax.fori_loop(0, rows, rel_block, 0, unroll=short)

    arrive(WHA, WHB, WHO, WP, PB)
    wha_v[...] = (wha_v[...].astype(f32) * 0.5).astype(bf16)
    bins = wp_v.shape[0]
    bias_col = column(pb_v[...])
    centers = (lax.broadcasted_iota(jnp.int32, (bins, 1), 0).astype(f32) + 0.5) * (32.0 / bins)
    arrive(WV, WO, WMB, WMA)
    wab_v[:, :width] = wmb_v[...]
    wab_v[:, width:] = wma_v[...]
    wab_sum = mm(jnp.ones((rows, inner), bf16), wab_v[...])

    pair_r[me] = pair_v[pl.ds(first, rows)]

    def take_single(k):
        if k == 0:
            if pairs > 1:
                landed = norm_r.at[pl.ds(0, pairs - 1)]
                pltpu.make_async_copy(landed, landed, recv_sem.at[0, 0]).wait()
            pltpu.make_async_copy(norm_s, norm_s, recv_sem.at[5, 0]).wait()
        else:
            half = norm_r.at[pl.ds(groups[k] * pairs, pairs), side]
            pltpu.make_async_copy(half, half, recv_sem.at[0, k]).wait()
            remote(half, half, 4, k, partner)

    send_pair_either(3, 2)
    send_pair(1)
    send_pair(0)
    for k in range(parts):
        take_single(k)
    for k in range(1, parts):
        half = norm_r.at[pl.ds(0, pairs), 0]
        pltpu.make_async_copy(half, half, recv_sem.at[4, k]).wait()
    every = norm_r[...].astype(f32).reshape(count, inner).astype(bf16)
    scores = mm(every, toward)
    values = mm(every, wv_v[...]).astype(bf16)
    for k in range(parts):
        take(bias_r, recv_sem.at[1], k)
    scores = scores + bias_r[...].astype(f32).reshape(count, spots) + mask_v[...]
    expo = jnp.exp(scores - jnp.max(scores, axis=0, keepdims=True))
    weights = (expo * (1.0 / jnp.sum(expo, axis=0, keepdims=True))).astype(bf16)
    mixed_heads = mm_tn(weights, values)
    attended = jnp.concatenate(
        [jnp.sum(jnp.where(own_head, mixed_heads[q * heads:(q + 1) * heads, :], 0.0),
                 axis=0, keepdims=True) for q in range(rows)], axis=0)
    refined = (mine + mm((gating * attended).astype(bf16), wo_v[...])).astype(bf16)
    raw = mm(refined, wab_v[...])
    exact = refined.astype(f32)
    middle = jnp.mean(exact, axis=-1, keepdims=True)
    away = exact - middle
    scale = lax.rsqrt(jnp.mean(away * away, axis=-1, keepdims=True) + epsilon)
    factors = ((raw - middle * wab_sum) * scale).astype(bf16)
    factor_b = factors[:, :width]
    b_s[...] = factor_b
    a_v[...] = factors[:, width:].astype(f32)
    b_r[me] = factor_b
    refined_ref[...] = refined

    for k in reversed(range(parts)):
        each_peer(k, lambda peer: remote(b_s, b_r.at[me], 3, k, peer))
    send_pair_either(2, 3)

    per = step // sub
    lane_part = lax.broadcasted_iota(jnp.int32, (rows, step), 1) // sub
    row_part = lax.broadcasted_iota(jnp.int32, (rows, step), 0) % per
    row_block = lax.broadcasted_iota(jnp.int32, (rows, step), 0) // per
    block = rows * sub

    def place_of(k, off):
        return pl.multiple_of(groups[k] * span + off, sub)

    def mix(k, off):
        at = place_of(k, off)
        near = pl.ds(at // rows, sub // rows)
        factor = b_r[near].astype(f32).reshape(sub, width)
        for q in range(rows):
            flat = (pin_v[q, pl.ds(at, sub), :] + pair_r[near, q].astype(f32).reshape(sub, width)
                    + a_v[q:q + 1, :] * factor)
            row = k * block + q * sub
            flat_v[row:row + sub, :] = flat
            x_v[row:row + sub, :] = norm_rows(flat).astype(bf16)

    def expand(ks):
        cut = 256
        for c in range(0, wha_v.shape[1], cut):
            wa = wha_v[:, c:c + cut]
            wb = whb_v[:, c:c + cut]
            for k in ks:
                for r in range(k * block, (k + 1) * block, step):
                    x = x_v[r:r + step, :]
                    half = mm(x, wa)
                    up = mm(x, wb)
                    hid_v[r:r + step, c:c + cut] = ((half + half * jnp.tanh(half)) * up).astype(bf16)

    def reduce(k):
        for r in range(k * block, (k + 1) * block, step):
            updated = flat_v[r:r + step, :] + mm(hid_v[r:r + step, :], who_v[...])
            x_v[r:r + step, :] = norm_rows(updated).astype(bf16)

    def grade(k, off):
        found = jnp.zeros((rows, step), f32)
        for v in range(rows // per):
            r = k * block + v * step
            logits = mm_nt(wp_v[...], x_v[r:r + step, :]) + bias_col
            expo = jnp.exp(logits - jnp.max(logits, axis=0, keepdims=True))
            value = (jnp.sum(expo * centers, axis=0, keepdims=True)
                     / jnp.sum(expo, axis=0, keepdims=True))
            found = jnp.where(row_block == v, value, found)
        spread = found
        for u in range(1, per):
            spread = jnp.where((lane_part + per - row_part) % per == u,
                               pltpu.roll(found, u * sub, 1), spread)
        at = place_of(k, off)
        where = pl.ds(pl.multiple_of(at // step * step, step), step)
        errors_ref[:, where] = jnp.where(
            lane_part == (at // sub) % per, spread, errors_ref[:, where])

    def ready(k):
        take(pair_r, recv_sem.at[2], k)
        take(b_r, recv_sem.at[3], k)

    errors_ref[...] = jnp.zeros_like(errors_ref)
    if short and parts == 4:
        take(b_r, recv_sem.at[3], 0)
        take(pair_r, recv_sem.at[2], 0)
        take(b_r, recv_sem.at[3], 1)
        take(pair_r, recv_sem.at[2], 1)
        mix(0, 0)
        mix(1, 0)
        expand((0,))
        expand((1,))
        reduce(0)
        reduce(1)
        take(b_r, recv_sem.at[3], 2)
        take(pair_r, recv_sem.at[2], 2)
        take(b_r, recv_sem.at[3], 3)
        take(pair_r, recv_sem.at[2], 3)
        mix(2, 0)
        grade(0, 0)
        mix(3, 0)
        expand((2,))
        grade(1, 0)
        expand((3,))
        reduce(2)
        reduce(3)
        grade(2, 0)
        grade(3, 0)
    else:
        for k in range(parts):
            ready(k)

        def more(c, _):
            for k in range(parts):
                mix(k, c * sub)
                expand((k,))
                reduce(k)
                grade(k, c * sub)
            return 0

        lax.fori_loop(0, span // sub, more, 0)

    def sent(buf, i, amount):
        out = buf.at[pl.ds(0, amount)]
        pltpu.make_async_copy(out, out, send_sem.at[i]).wait()

    sent(bias_r, 1, n - 1)
    sent(pair_r, 2, n - 1)
    sent(b_r, 3, n - 1)
    pltpu.make_async_copy(norm_s, norm_s, send_sem.at[5]).wait()
    if n > 2:
        sent(norm_r, 0, (size - 2 + (parts - 1) * pairs) // 2)
    if parts > 1:
        sent(norm_r, 4, (parts - 1) * pairs // 2)


def place(refined_v, errors_v, refined_h, errors_h, sem):
    copies = (
        pltpu.make_async_copy(refined_v, refined_h, sem.at[0]),
        pltpu.make_async_copy(errors_v, errors_h, sem.at[1]),
    )
    for copy in copies:
        copy.start()
    for copy in copies:
        copy.wait()


def on_device(n, pair_repr, single_repr, residue_index, chain_index, complex_index, pad_mask,
              w_query, w_key, w_value, w_gate, w_out, w_bias, rel_table, w_mix_a, w_mix_b,
              w_hidden_a, w_hidden_b, w_hidden_out, w_pae, pae_bias):
    count, rows, width = pair_repr.shape
    inner = single_repr.shape[1]
    heads = w_bias.shape[1]
    hidden = w_hidden_a.shape[1]
    args = (pair_repr, single_repr, residue_index[None], chain_index[None], complex_index[None],
            pad_mask[None], w_query, w_key, w_value, w_gate, w_out, w_bias.T, rel_table,
            w_mix_a, w_mix_b, w_hidden_a, w_hidden_b, w_hidden_out, w_pae.T, pae_bias[None])
    spots = rows * heads
    step = min(count, 128)
    scratch = [pltpu.VMEM(a.shape, a.dtype) for a in args] + [
        pltpu.VMEM((count, 128), f32),
        pltpu.VMEM((count, 128), f32),
        pltpu.VMEM((count, spots), f32),
        pltpu.VMEM((n, rows, spots), bf16),
        pltpu.VMEM((n, rows, spots), bf16),
        pltpu.VMEM((rows, inner), bf16),
        pltpu.VMEM((n // 2, 2, rows, inner), bf16),
        pltpu.VMEM((n, rows, rows, width), bf16),
        pltpu.VMEM((rows, width), bf16),
        pltpu.VMEM((n, rows, width), bf16),
        pltpu.VMEM((rows, width), f32),
        pltpu.VMEM((rows, count, width), f32),
        pltpu.VMEM((rows * step, width), f32),
        pltpu.VMEM((rows * step, width), bf16),
        pltpu.VMEM((rows * step, hidden), bf16),
        pltpu.VMEM((inner, 2 * width), bf16),
        pltpu.SemaphoreType.DMA((len(args),)),
        pltpu.SemaphoreType.DMA((6,)),
        pltpu.SemaphoreType.DMA((6, 4)),
    ]
    refined, errors = pl.pallas_call(
        functools.partial(kernel, n, heads),
        out_shape=(pltpu.VMEM((rows, inner), bf16), pltpu.VMEM((rows, count), f32)),
        in_specs=[pl.BlockSpec(memory_space=pltpu.HBM)] * len(args),
        out_specs=[pl.BlockSpec(memory_space=pltpu.VMEM)] * 2,
        scratch_shapes=scratch,
        compiler_params=pltpu.CompilerParams(
            collective_id=0, has_side_effects=True, vmem_limit_bytes=40 * 1024 * 1024),
        name="confidence",
    )(*[pltpu.with_memory_space_constraint(a, pltpu.HBM) for a in args])
    return pl.pallas_call(
        place,
        out_shape=(
            jax.ShapeDtypeStruct((rows, inner), bf16),
            jax.ShapeDtypeStruct((rows, count), f32),
        ),
        in_specs=[pl.BlockSpec(memory_space=pltpu.VMEM)] * 2,
        out_specs=[pl.BlockSpec(memory_space=pltpu.HBM)] * 2,
        scratch_shapes=[pltpu.SemaphoreType.DMA((2,))],
        compiler_params=pltpu.CompilerParams(vmem_limit_bytes=1024 * 1024),
        name="place",
    )(refined, errors)


def solution(mesh):
    placed = (
        P("groups", "rows", None),
        P(("groups", "rows"), None),
        P("groups"),
        P("groups"),
        P("groups"),
        P("groups"),
    ) + (P(),) * 14
    return jax.shard_map(
        functools.partial(on_device, mesh.shape["rows"]),
        mesh=mesh,
        in_specs=placed,
        out_specs=(P(("groups", "rows"), None), P(("groups", "rows"), None)),
        check_vma=False,
    )
```

```python
import functools
import math

import jax
import jax.numpy as jnp
from jax import lax
from jax.experimental import pallas as pl
from jax.experimental.pallas import tpu as pltpu
from jax.sharding import PartitionSpec as P

epsilon = 1e-05
masked_score = -1e30
chain_step = 65536.0
f32 = jnp.float32
bf16 = jnp.bfloat16


def norm_rows(values):
    center = values - jnp.mean(values, axis=-1, keepdims=True)
    spread = jnp.mean(center * center, axis=-1, keepdims=True)
    return center * lax.rsqrt(spread + epsilon)


def mm(a, b):
    return jnp.dot(a, b, preferred_element_type=f32)


def mm_nt(a, b):
    return lax.dot_general(a, b, (((1,), (1,)), ((), ())), preferred_element_type=f32)


def mm_tn(a, b):
    return lax.dot_general(a, b, (((0,), (0,)), ((), ())), preferred_element_type=f32)


def column(row):
    m = row.shape[1]
    pick = lax.broadcasted_iota(jnp.int32, (m, m), 0) == lax.broadcasted_iota(jnp.int32, (m, m), 1)
    return jnp.sum(jnp.where(pick, row, 0.0), axis=1, keepdims=True)


def bucket_onehot(diff, classes):
    reach = (classes - 2) // 2
    same = jnp.abs(diff) < 0.5 * chain_step
    bucket = jnp.where(same, jnp.clip(diff, -reach, reach) + reach, 2.0 * reach + 1.0)
    lanes = lax.broadcasted_iota(jnp.int32, bucket.shape, bucket.ndim - 1).astype(f32)
    return jnp.where(bucket == lanes, 1.0, 0.0).astype(bf16)


def kernel(
    n,
    heads,
    pair_h, single_h, res_h, chain_h, complex_h, pad_h,
    wq_h, wk_h, wv_h, wg_h, wo_h, wb_h, rel_h, wma_h, wmb_h, wha_h, whb_h, who_h, wp_h, pb_h,
    refined_ref, errors_ref,
    pair_v, single_v, res_v, chain_v, complex_v, pad_v,
    wq_v, wk_v, wv_v, wg_v, wo_v, wb_v, rel_v, wma_v, wmb_v, wha_v, whb_v, who_v, wp_v, pb_v,
    code_v, ccol_v, mask_v, bias_s, bias_r, norm_s, norm_r, pair_r, b_s, b_r, a_v, pin_v,
    flat_v, x_v, hid_v, wab_v, scale_v, square_v,
    local_sem, send_sem, recv_sem,
):
    me = lax.axis_index("rows")
    count, rows, width = pair_h.shape
    classes = rel_h.shape[0]
    inner = single_h.shape[1]
    head_size = inner // heads
    spots = rows * heads
    first = pl.multiple_of(me * rows, rows)
    step = min(count, 128)
    short = count == step
    sub = 32

    hbm = (pair_h, single_h, res_h, chain_h, complex_h, pad_h, wq_h, wk_h, wv_h, wg_h, wo_h,
           wb_h, rel_h, wma_h, wmb_h, wha_h, whb_h, who_h, wp_h, pb_h)
    vmem = (pair_v, single_v, res_v, chain_v, complex_v, pad_v, wq_v, wk_v, wv_v, wg_v, wo_v,
            wb_v, rel_v, wma_v, wmb_v, wha_v, whb_v, who_v, wp_v, pb_v)
    (PAIR, SINGLE, RES, CHAIN, COMPLEX, PAD, WQ, WK, WV, WG, WO, WB, REL, WMA, WMB, WHA, WHB,
     WHO, WP, PB) = range(len(hbm))
    loads = [pltpu.make_async_copy(h, v, local_sem.at[i]) for i, (h, v) in enumerate(zip(hbm, vmem))]

    def arrive(*which):
        for i in which:
            loads[i].wait()

    parts = 4 if n % 4 == 0 else 1
    size = n // parts
    mine_at = me % size
    group = me // size
    low = group % 2
    groups = (group, group + 1 - 2 * low, group + 2 - 4 * (group // 2), 3 - group)[:parts]
    span = size * rows

    def each_peer(k, visit):
        base = groups[k] * size

        def body(s, _):
            visit(base + (mine_at + s) % size)
            return 0

        if short:
            for s in range(1 if k == 0 else 0, size):
                body(s, 0)
        else:
            lax.fori_loop(1 if k == 0 else 0, size, body, 0)

    def take(buf, sems, k):
        landed = buf.at[pl.ds(0, size - (1 if k == 0 else 0))]
        pltpu.make_async_copy(landed, landed, sems.at[k]).wait()

    for i in (RES, CHAIN, SINGLE):
        loads[i].start()
    barrier = pltpu.get_barrier_semaphore()
    for k in reversed(range(parts)):
        each_peer(k, lambda peer: pl.semaphore_signal(
            barrier, inc=1, device_id={"rows": peer}, device_id_type=pl.DeviceIdType.MESH))
    for i in (REL, WB, PAIR, COMPLEX, PAD, WQ, WG, WK, WV, WO, WMB, WMA, WHA, WHB, WHO, WP, PB):
        loads[i].start()

    arrive(RES, CHAIN)
    for k in range(0, count, step):
        code = chain_v[:, k:k + step].astype(f32) * chain_step + res_v[:, k:k + step].astype(f32)
        code_v[k:k + step, :] = jnp.broadcast_to(column(code), (step, 128))

    arrive(SINGLE)
    mine = single_v[...].astype(f32)
    center = jnp.mean(mine, axis=-1, keepdims=True)
    normed = norm_rows(mine).astype(bf16)
    norm_s[...] = normed
    norm_r[me // 2, me % 2] = normed

    arrive(REL, WB, PAIR)
    rel = rel_v[...]
    tile_h = jnp.where(
        lax.broadcasted_iota(jnp.int32, (heads, spots), 1) % heads
        == lax.broadcasted_iota(jnp.int32, (heads, spots), 0), 1.0, 0.0).astype(bf16)
    w_tiled = mm_tn(wb_v[...], tile_h).astype(bf16)
    code_keys = code_v[pl.ds(first, rows), :classes]

    def bias_block(j, _):
        at = pl.multiple_of(j * step, step)
        code_i = code_v[pl.ds(at, step), :classes]
        diff = code_i[:, None, :] - code_keys[None, :, :]
        hot = bucket_onehot(diff.reshape(step * rows, classes), classes)
        cells = mm(hot, rel) + pair_v[pl.ds(at, step)].astype(f32).reshape(step * rows, width)
        out = mm(norm_rows(cells).astype(bf16), w_tiled)
        out = out.reshape(step // rows, rows, rows, spots)
        lane_q = lax.broadcasted_iota(jnp.int32, (1, 1, spots), 2) // heads
        total = jnp.where(lane_q == 0, out[:, 0], 0.0)
        for q in range(1, rows):
            total = jnp.where(lane_q == q, out[:, q], total)
        bias_s[pl.ds(pl.multiple_of(j * (step // rows), step // rows), step // rows)] = total.astype(bf16)
        return 0

    lax.fori_loop(0, count // step, bias_block, 0, unroll=short)
    bias_r[me] = bias_s[me]

    pl.semaphore_wait(barrier, n - 1)

    def remote(src, dst, i, k, peer):
        pltpu.make_async_remote_copy(
            src_ref=src, dst_ref=dst, send_sem=send_sem.at[i], recv_sem=recv_sem.at[i, k],
            device_id={"rows": peer}, device_id_type=pl.DeviceIdType.MESH).start()

    side = me % 2
    partner = me + 1 - 2 * side
    pairs = size // 2

    def spread_single(k):
        base = groups[k] * size

        def body(s, _):
            chip = base + 2 * ((mine_at // 2 + s) % pairs)
            for core in (0, 1) if k == 0 else (side,):
                remote(norm_s, norm_r.at[me // 2, side], 0, k, chip + core)
            return 0

        if short:
            for s in range(1 if k == 0 else 0, pairs):
                body(s, 0)
        else:
            lax.fori_loop(1 if k == 0 else 0, pairs, body, 0)
        if k == 0:
            remote(norm_s, norm_r.at[me // 2, side], 5, 0, partner)

    for k in reversed(range(parts)):
        spread_single(k)
    for k in reversed(range(parts)):
        each_peer(k, lambda peer: remote(bias_s.at[peer], bias_r.at[me], 1, k, peer))

    def send_pair(k):
        each_peer(k, lambda peer: remote(
            pair_v.at[pl.ds(peer * rows, rows)], pair_r.at[me], 2, k, peer))

    def send_pair_either(edge, middle):
        inside = group * (3 - group) // 2
        k = edge + (middle - edge) * inside
        base = (groups[edge] + (groups[middle] - groups[edge]) * inside) * size
        for s in range(size) if short else ():
            peer = base + (mine_at + s) % size
            remote(pair_v.at[pl.ds(peer * rows, rows)], pair_r.at[me], 2, k, peer)
        if not short:
            def body(s, _):
                peer = base + (mine_at + s) % size
                remote(pair_v.at[pl.ds(peer * rows, rows)], pair_r.at[me], 2, k, peer)
                return 0

            lax.fori_loop(0, size, body, 0)

    arrive(WQ)
    queries = mm(normed, wq_v[...]).astype(bf16).astype(f32)
    arrive(WG)
    gating = jax.nn.sigmoid(mm(normed, wg_v[...]))
    head_of = lax.broadcasted_iota(jnp.int32, (heads, inner), 1) // head_size
    own_head = head_of == lax.broadcasted_iota(jnp.int32, (heads, inner), 0)
    q_wide = jnp.concatenate(
        [jnp.where(own_head, queries[q:q + 1, :], 0.0) for q in range(rows)], axis=0).astype(bf16)
    arrive(WK)
    toward = (mm_nt(wk_v[...], q_wide) / math.sqrt(head_size)).astype(bf16)

    arrive(COMPLEX, PAD)
    lane_spot = lax.broadcasted_iota(jnp.int32, (step, spots), 1) // heads
    for k in range(0, count, step):
        ccol_v[k:k + step, :] = jnp.broadcast_to(
            column(complex_v[:, k:k + step].astype(f32)), (step, 128))
    mine_c = ccol_v[pl.ds(first, rows), 0:1]
    lane_row = lax.broadcasted_iota(jnp.int32, (rows, spots), 1) // heads
    pick = lane_row == lax.broadcasted_iota(jnp.int32, (rows, spots), 0)
    query_c = jnp.sum(jnp.where(pick, mine_c, 0.0), axis=0, keepdims=True)
    for k in range(0, count, step):
        real = column(pad_v[:, k:k + step].astype(f32)) == 1.0
        same = ccol_v[k:k + step, :spots] == query_c
        itself = (lax.broadcasted_iota(jnp.int32, (step, spots), 0) + k) == (first + lane_spot)
        mask_v[k:k + step, :] = jnp.where(same & (real | itself), 0.0, masked_score)

    def rel_block(q, _):
        diff = code_v[pl.ds(first + q, 1), :classes] - code_v[:, :classes]
        pin_v[q] = mm(bucket_onehot(diff, classes), rel)
        return 0

    lax.fori_loop(0, rows, rel_block, 0, unroll=short)

    arrive(WHA, WHB, WHO, WP, PB)
    wha_v[...] = (wha_v[...].astype(f32) * 0.5).astype(bf16)
    down = who_v[...].astype(f32)
    who_v[...] = (down - jnp.mean(down, axis=-1, keepdims=True)).astype(bf16)
    bins = wp_v.shape[0]
    bias_col = column(pb_v[...])
    even = jnp.full((8, width), 1.0 / width, bf16)
    centers = (lax.broadcasted_iota(jnp.int32, (bins, 1), 0).astype(f32) + 0.5) * (32.0 / bins)
    arrive(WV, WO, WMB, WMA)
    wab_v[:, :width] = wmb_v[...]
    wab_v[:, width:] = wma_v[...]
    wab_sum = mm(jnp.ones((rows, inner), bf16), wab_v[...])

    pair_r[me] = pair_v[pl.ds(first, rows)]

    def take_single(k):
        if k == 0:
            if pairs > 1:
                landed = norm_r.at[pl.ds(0, pairs - 1)]
                pltpu.make_async_copy(landed, landed, recv_sem.at[0, 0]).wait()
            pltpu.make_async_copy(norm_s, norm_s, recv_sem.at[5, 0]).wait()
        else:
            half = norm_r.at[pl.ds(groups[k] * pairs, pairs), side]
            pltpu.make_async_copy(half, half, recv_sem.at[0, k]).wait()
            remote(half, half, 4, k, partner)

    send_pair_either(3, 2)
    send_pair(1)
    send_pair(0)
    for k in range(parts):
        take_single(k)
    for k in range(1, parts):
        half = norm_r.at[pl.ds(0, pairs), 0]
        pltpu.make_async_copy(half, half, recv_sem.at[4, k]).wait()
    every = norm_r[...].astype(f32).reshape(count, inner).astype(bf16)
    scores = mm(every, toward)
    values = mm(every, wv_v[...]).astype(bf16)
    for k in range(parts):
        take(bias_r, recv_sem.at[1], k)
    scores = scores + bias_r[...].astype(f32).reshape(count, spots) + mask_v[...]
    expo = jnp.exp(scores - jnp.max(scores, axis=0, keepdims=True))
    weights = (expo * (1.0 / jnp.sum(expo, axis=0, keepdims=True))).astype(bf16)
    mixed_heads = mm_tn(weights, values)
    attended = jnp.concatenate(
        [jnp.sum(jnp.where(own_head, mixed_heads[q * heads:(q + 1) * heads, :], 0.0),
                 axis=0, keepdims=True) for q in range(rows)], axis=0)
    refined = (mine + mm((gating * attended).astype(bf16), wo_v[...])).astype(bf16)
    raw = mm(refined, wab_v[...])
    exact = refined.astype(f32)
    away = exact - center
    shift = jnp.mean(away, axis=-1, keepdims=True)
    spread = jnp.maximum(jnp.mean(away * away, axis=-1, keepdims=True) - shift * shift, 0.0)
    middle = center + shift
    scale = lax.rsqrt(spread + epsilon)
    factors = ((raw - middle * wab_sum) * scale).astype(bf16)
    factor_b = factors[:, :width]
    b_s[...] = factor_b
    a_v[...] = factors[:, width:].astype(f32)
    b_r[me] = factor_b
    refined_ref[...] = refined

    for k in reversed(range(parts)):
        each_peer(k, lambda peer: remote(b_s, b_r.at[me], 3, k, peer))
    send_pair_either(2, 3)

    per = step // sub
    lane_part = lax.broadcasted_iota(jnp.int32, (rows, step), 1) // sub
    row_part = lax.broadcasted_iota(jnp.int32, (rows, step), 0) % per
    row_block = lax.broadcasted_iota(jnp.int32, (rows, step), 0) // per
    block = rows * sub

    def place_of(k, off):
        return pl.multiple_of(groups[k] * span + off, sub)

    def mix(k, off):
        at = place_of(k, off)
        near = pl.ds(at // rows, sub // rows)
        factor = b_r[near].astype(f32).reshape(sub, width)
        for q in range(rows):
            flat = (pin_v[q, pl.ds(at, sub), :] + pair_r[near, q].astype(f32).reshape(sub, width)
                    + a_v[q:q + 1, :] * factor)
            row = k * block + q * sub
            center = flat - jnp.mean(flat, axis=-1, keepdims=True)
            spread = jnp.mean(center * center, axis=-1, keepdims=True)
            flat_v[row:row + sub, :] = center
            x_v[row:row + sub, :] = center.astype(bf16)
            scale_v[row:row + sub, :] = jnp.broadcast_to(lax.rsqrt(spread + epsilon), (sub, 128))

    def expand(ks):
        cut = 256
        for c in range(0, wha_v.shape[1], cut):
            wa = wha_v[:, c:c + cut]
            wb = whb_v[:, c:c + cut]
            for k in ks:
                for r in range(k * block, (k + 1) * block, step):
                    x = x_v[r:r + step, :]
                    scale = jnp.tile(scale_v[r:r + step, :], (1, cut // 128))
                    half = mm(x, wa) * scale
                    up = mm(x, wb) * scale
                    hid_v[r:r + step, c:c + cut] = ((half + half * jnp.tanh(half)) * up).astype(bf16)

    def reduce(k):
        for r in range(k * block, (k + 1) * block, step):
            center = flat_v[r:r + step, :] + mm(hid_v[r:r + step, :], who_v[...])
            x_v[r:r + step, :] = center.astype(bf16)
            square_v[r:r + step, :] = (center * center).astype(bf16)

    def grade(k, off):
        found = jnp.zeros((rows, step), f32)
        for v in range(rows // per):
            r = k * block + v * step
            spread = mm_nt(even, square_v[r:r + step, :])[0:1]
            logits = mm_nt(wp_v[...], x_v[r:r + step, :]) * lax.rsqrt(spread + epsilon) + bias_col
            expo = jnp.exp(logits - jnp.max(logits, axis=0, keepdims=True))
            value = (jnp.sum(expo * centers, axis=0, keepdims=True)
                     / jnp.sum(expo, axis=0, keepdims=True))
            found = jnp.where(row_block == v, value, found)
        spread = found
        for u in range(1, per):
            spread = jnp.where((lane_part + per - row_part) % per == u,
                               pltpu.roll(found, u * sub, 1), spread)
        at = place_of(k, off)
        where = pl.ds(pl.multiple_of(at // step * step, step), step)
        errors_ref[:, where] = jnp.where(
            lane_part == (at // sub) % per, spread, errors_ref[:, where])

    def ready(k):
        take(pair_r, recv_sem.at[2], k)
        take(b_r, recv_sem.at[3], k)

    errors_ref[...] = jnp.zeros_like(errors_ref)
    if short and parts == 4:
        take(b_r, recv_sem.at[3], 0)
        take(pair_r, recv_sem.at[2], 0)
        take(b_r, recv_sem.at[3], 1)
        take(pair_r, recv_sem.at[2], 1)
        mix(0, 0)
        mix(1, 0)
        expand((0,1,))
        reduce(0)
        reduce(1)
        take(b_r, recv_sem.at[3], 2)
        take(pair_r, recv_sem.at[2], 2)
        mix(2, 0)
        grade(0, 0)
        grade(1, 0)
        expand((2,))
        take(b_r, recv_sem.at[3], 3)
        take(pair_r, recv_sem.at[2], 3)
        mix(3, 0)
        reduce(2)
        expand((3,))
        grade(2, 0)
        reduce(3)
        grade(3, 0)
    else:
        for k in range(parts):
            ready(k)

        def more(c, _):
            for k in range(parts):
                mix(k, c * sub)
                expand((k,))
                reduce(k)
                grade(k, c * sub)
            return 0

        lax.fori_loop(0, span // sub, more, 0)

    def sent(buf, i, amount):
        out = buf.at[pl.ds(0, amount)]
        pltpu.make_async_copy(out, out, send_sem.at[i]).wait()

    sent(bias_r, 1, n - 1)
    sent(pair_r, 2, n - 1)
    sent(b_r, 3, n - 1)
    pltpu.make_async_copy(norm_s, norm_s, send_sem.at[5]).wait()
    if n > 2:
        sent(norm_r, 0, (size - 2 + (parts - 1) * pairs) // 2)
    if parts > 1:
        sent(norm_r, 4, (parts - 1) * pairs // 2)


def place(refined_v, errors_v, refined_h, errors_h, sem):
    copies = (
        pltpu.make_async_copy(refined_v, refined_h, sem.at[0]),
        pltpu.make_async_copy(errors_v, errors_h, sem.at[1]),
    )
    for copy in copies:
        copy.start()
    for copy in copies:
        copy.wait()


def on_device(n, pair_repr, single_repr, residue_index, chain_index, complex_index, pad_mask,
              w_query, w_key, w_value, w_gate, w_out, w_bias, rel_table, w_mix_a, w_mix_b,
              w_hidden_a, w_hidden_b, w_hidden_out, w_pae, pae_bias):
    count, rows, width = pair_repr.shape
    inner = single_repr.shape[1]
    heads = w_bias.shape[1]
    hidden = w_hidden_a.shape[1]
    args = (pair_repr, single_repr, residue_index[None], chain_index[None], complex_index[None],
            pad_mask[None], w_query, w_key, w_value, w_gate, w_out, w_bias.T, rel_table,
            w_mix_a, w_mix_b, w_hidden_a, w_hidden_b, w_hidden_out, w_pae.T, pae_bias[None])
    spots = rows * heads
    step = min(count, 128)
    scratch = [pltpu.VMEM(a.shape, a.dtype) for a in args] + [
        pltpu.VMEM((count, 128), f32),
        pltpu.VMEM((count, 128), f32),
        pltpu.VMEM((count, spots), f32),
        pltpu.VMEM((n, rows, spots), bf16),
        pltpu.VMEM((n, rows, spots), bf16),
        pltpu.VMEM((rows, inner), bf16),
        pltpu.VMEM((n // 2, 2, rows, inner), bf16),
        pltpu.VMEM((n, rows, rows, width), bf16),
        pltpu.VMEM((rows, width), bf16),
        pltpu.VMEM((n, rows, width), bf16),
        pltpu.VMEM((rows, width), f32),
        pltpu.VMEM((rows, count, width), f32),
        pltpu.VMEM((rows * step, width), f32),
        pltpu.VMEM((rows * step, width), bf16),
        pltpu.VMEM((rows * step, hidden), bf16),
        pltpu.VMEM((inner, 2 * width), bf16),
        pltpu.VMEM((rows * step, 128), f32),
        pltpu.VMEM((rows * step, width), bf16),
        pltpu.SemaphoreType.DMA((len(args),)),
        pltpu.SemaphoreType.DMA((6,)),
        pltpu.SemaphoreType.DMA((6, 4)),
    ]
    refined, errors = pl.pallas_call(
        functools.partial(kernel, n, heads),
        out_shape=(pltpu.VMEM((rows, inner), bf16), pltpu.VMEM((rows, count), f32)),
        in_specs=[pl.BlockSpec(memory_space=pltpu.HBM)] * len(args),
        out_specs=[pl.BlockSpec(memory_space=pltpu.VMEM)] * 2,
        scratch_shapes=scratch,
        compiler_params=pltpu.CompilerParams(
            collective_id=0, has_side_effects=True, vmem_limit_bytes=40 * 1024 * 1024),
        name="confidence",
    )(*[pltpu.with_memory_space_constraint(a, pltpu.HBM) for a in args])
    return pl.pallas_call(
        place,
        out_shape=(
            jax.ShapeDtypeStruct((rows, inner), bf16),
            jax.ShapeDtypeStruct((rows, count), f32),
        ),
        in_specs=[pl.BlockSpec(memory_space=pltpu.VMEM)] * 2,
        out_specs=[pl.BlockSpec(memory_space=pltpu.HBM)] * 2,
        scratch_shapes=[pltpu.SemaphoreType.DMA((2,))],
        compiler_params=pltpu.CompilerParams(vmem_limit_bytes=1024 * 1024),
        name="place",
    )(refined, errors)


def solution(mesh):
    placed = (
        P("groups", "rows", None),
        P(("groups", "rows"), None),
        P("groups"),
        P("groups"),
        P("groups"),
        P("groups"),
    ) + (P(),) * 14
    return jax.shard_map(
        functools.partial(on_device, mesh.shape["rows"]),
        mesh=mesh,
        in_specs=placed,
        out_specs=(P(("groups", "rows"), None), P(("groups", "rows"), None)),
        check_vma=False,
    )
```

```python
import functools
import math

import jax
import jax.numpy as jnp
from jax import lax
from jax.experimental import pallas as pl
from jax.experimental.pallas import tpu as pltpu
from jax.sharding import PartitionSpec as P

epsilon = 1e-05
masked_score = -1e30
chain_step = 65536.0
f32 = jnp.float32
bf16 = jnp.bfloat16


def norm_rows(values):
    center = values - jnp.mean(values, axis=-1, keepdims=True)
    spread = jnp.mean(center * center, axis=-1, keepdims=True)
    return center * lax.rsqrt(spread + epsilon)


def mm(a, b):
    return jnp.dot(a, b, preferred_element_type=f32)


def mm_nt(a, b):
    return lax.dot_general(a, b, (((1,), (1,)), ((), ())), preferred_element_type=f32)


def mm_tn(a, b):
    return lax.dot_general(a, b, (((0,), (0,)), ((), ())), preferred_element_type=f32)


def column(row):
    m = row.shape[1]
    pick = lax.broadcasted_iota(jnp.int32, (m, m), 0) == lax.broadcasted_iota(jnp.int32, (m, m), 1)
    return jnp.sum(jnp.where(pick, row, 0.0), axis=1, keepdims=True)


def bucket_onehot(diff, classes):
    reach = (classes - 2) // 2
    same = jnp.abs(diff) < 0.5 * chain_step
    bucket = jnp.where(same, jnp.clip(diff, -reach, reach) + reach, 2.0 * reach + 1.0)
    lanes = lax.broadcasted_iota(jnp.int32, bucket.shape, bucket.ndim - 1).astype(f32)
    return jnp.where(bucket == lanes, 1.0, 0.0).astype(bf16)


def kernel(
    n,
    heads,
    pair_h, single_h, res_h, chain_h, complex_h, pad_h,
    wq_h, wk_h, wv_h, wg_h, wo_h, wb_h, rel_h, wma_h, wmb_h, wha_h, whb_h, who_h, wp_h, pb_h,
    refined_ref, errors_ref,
    pair_v, single_v, res_v, chain_v, complex_v, pad_v,
    wq_v, wk_v, wv_v, wg_v, wo_v, wb_v, rel_v, wma_v, wmb_v, wha_v, whb_v, who_v, wp_v, pb_v,
    code_v, ccol_v, mask_v, bias_s, bias_r, norm_s, norm_r, pair_r, b_s, b_r, a_v, pin_v,
    flat_v, x_v, hid_v, wab_v, scale_v, square_v, score_v,
    local_sem, send_sem, recv_sem,
):
    me = lax.axis_index("rows")
    count, rows, width = pair_h.shape
    classes = rel_h.shape[0]
    inner = single_h.shape[1]
    head_size = inner // heads
    spots = rows * heads
    first = pl.multiple_of(me * rows, rows)
    step = min(count, 128)
    short = count == step
    sub = 32

    hbm = (pair_h, single_h, res_h, chain_h, complex_h, pad_h, wq_h, wk_h, wv_h, wg_h, wo_h,
           wb_h, rel_h, wma_h, wmb_h, wha_h, whb_h, who_h, wp_h, pb_h)
    vmem = (pair_v, single_v, res_v, chain_v, complex_v, pad_v, wq_v, wk_v, wv_v, wg_v, wo_v,
            wb_v, rel_v, wma_v, wmb_v, wha_v, whb_v, who_v, wp_v, pb_v)
    (PAIR, SINGLE, RES, CHAIN, COMPLEX, PAD, WQ, WK, WV, WG, WO, WB, REL, WMA, WMB, WHA, WHB,
     WHO, WP, PB) = range(len(hbm))
    loads = [pltpu.make_async_copy(h, v, local_sem.at[i]) for i, (h, v) in enumerate(zip(hbm, vmem))]

    def arrive(*which):
        for i in which:
            loads[i].wait()

    parts = 4 if n % 4 == 0 else 1
    size = n // parts
    mine_at = me % size
    group = me // size
    low = group % 2
    groups = (group, group + 1 - 2 * low, group + 2 - 4 * (group // 2), 3 - group)[:parts]
    span = size * rows

    def each_peer(k, visit):
        base = groups[k] * size

        def body(s, _):
            visit(base + (mine_at + s) % size)
            return 0

        if short:
            for s in range(1 if k == 0 else 0, size):
                body(s, 0)
        else:
            lax.fori_loop(1 if k == 0 else 0, size, body, 0)

    def take(buf, sems, k):
        landed = buf.at[pl.ds(0, size - (1 if k == 0 else 0))]
        pltpu.make_async_copy(landed, landed, sems.at[k]).wait()

    barrier = pltpu.get_barrier_semaphore()
    for k in reversed(range(parts)):
        each_peer(k, lambda peer: pl.semaphore_signal(
            barrier, inc=1, device_id={"rows": peer}, device_id_type=pl.DeviceIdType.MESH))
    for i in (RES, CHAIN, SINGLE, REL, WB, PAIR, COMPLEX, PAD, WQ, WG, WK, WV, WO, WMB, WMA, WHA, WHB, WHO, WP, PB):
        loads[i].start()

    arrive(RES, CHAIN)
    for k in range(0, count, step):
        code = chain_v[:, k:k + step].astype(f32) * chain_step + res_v[:, k:k + step].astype(f32)
        code_v[k:k + step, :] = jnp.broadcast_to(column(code), (step, 128))

    arrive(SINGLE)
    mine = single_v[...].astype(f32)
    center = jnp.mean(mine, axis=-1, keepdims=True)
    normed = norm_rows(mine).astype(bf16)
    norm_s[...] = normed
    norm_r[me // 2, me % 2] = normed

    arrive(REL, WB, PAIR)
    rel = rel_v[...]
    tile_h = jnp.where(
        lax.broadcasted_iota(jnp.int32, (heads, spots), 1) // rows
        == lax.broadcasted_iota(jnp.int32, (heads, spots), 0), 1.0, 0.0).astype(bf16)
    w_tiled = mm_tn(wb_v[...], tile_h).astype(bf16)
    code_keys = code_v[pl.ds(first, rows), :classes]

    def bias_block(j, _):
        at = pl.multiple_of(j * step, step)
        code_i = code_v[pl.ds(at, step), :classes]
        diff = code_i[:, None, :] - code_keys[None, :, :]
        hot = bucket_onehot(diff.reshape(step * rows, classes), classes)
        cells = mm(hot, rel) + pair_v[pl.ds(at, step)].astype(f32).reshape(step * rows, width)
        out = mm(norm_rows(cells).astype(bf16), w_tiled)
        out = out.reshape(step // rows, rows, rows, spots)
        lane_q = lax.broadcasted_iota(jnp.int32, (1, 1, spots), 2) % rows
        total = jnp.where(lane_q == 0, out[:, 0], 0.0)
        for q in range(1, rows):
            total = jnp.where(lane_q == q, out[:, q], total)
        bias_s[pl.ds(pl.multiple_of(j * (step // rows), step // rows), step // rows)] = total.astype(bf16)
        return 0

    lax.fori_loop(0, count // step, bias_block, 0, unroll=short)
    bias_r[me] = bias_s[me]

    pl.semaphore_wait(barrier, n - 1)

    def remote(src, dst, i, k, peer):
        pltpu.make_async_remote_copy(
            src_ref=src, dst_ref=dst, send_sem=send_sem.at[i], recv_sem=recv_sem.at[i, k],
            device_id={"rows": peer}, device_id_type=pl.DeviceIdType.MESH).start()

    side = me % 2
    partner = me + 1 - 2 * side
    pairs = size // 2

    def spread_single(k):
        base = groups[k] * size

        def body(s, _):
            chip = base + 2 * ((mine_at // 2 + s) % pairs)
            for core in (0, 1) if k == 0 else (side,):
                remote(norm_s, norm_r.at[me // 2, side], 0, k, chip + core)
            return 0

        if short:
            for s in range(1 if k == 0 else 0, pairs):
                body(s, 0)
        else:
            lax.fori_loop(1 if k == 0 else 0, pairs, body, 0)
        if k == 0:
            remote(norm_s, norm_r.at[me // 2, side], 5, 0, partner)

    for k in reversed(range(parts)):
        spread_single(k)
    for k in reversed(range(parts)):
        each_peer(k, lambda peer: remote(bias_s.at[peer], bias_r.at[me], 1, k, peer))

    def send_pair(k):
        each_peer(k, lambda peer: remote(
            pair_v.at[pl.ds(peer * rows, rows)], pair_r.at[me], 2, k, peer))

    def send_pair_either(edge, middle, low, high):
        inside = group * (3 - group) // 2
        k = edge + (middle - edge) * inside
        base = (groups[edge] + (groups[middle] - groups[edge]) * inside) * size

        def body(s, _):
            peer = base + (mine_at + s) % size
            remote(pair_v.at[pl.ds(peer * rows, rows)], pair_r.at[me], 2, k, peer)
            return 0

        if short:
            for s in range(low, high):
                body(s, 0)
        else:
            lax.fori_loop(low, high, body, 0)

    arrive(WQ)
    queries = mm(normed, wq_v[...]).astype(bf16).astype(f32)
    arrive(WG)
    gating = jax.nn.sigmoid(mm(normed, wg_v[...]))
    head_of = lax.broadcasted_iota(jnp.int32, (rows, inner), 1) // head_size
    q_wide = jnp.concatenate(
        [jnp.where(head_of == h, queries, 0.0) for h in range(heads)], axis=0).astype(bf16)
    arrive(WK)
    toward = (mm_nt(wk_v[...], q_wide) / math.sqrt(head_size)).astype(bf16)

    arrive(COMPLEX, PAD)
    lane_spot = lax.broadcasted_iota(jnp.int32, (step, spots), 1) % rows
    for k in range(0, count, step):
        ccol_v[k:k + step, :] = jnp.broadcast_to(
            column(complex_v[:, k:k + step].astype(f32)), (step, 128))
    mine_c = ccol_v[pl.ds(first, rows), 0:1]
    lane_row = lax.broadcasted_iota(jnp.int32, (rows, spots), 1) % rows
    pick = lane_row == lax.broadcasted_iota(jnp.int32, (rows, spots), 0)
    query_c = jnp.sum(jnp.where(pick, mine_c, 0.0), axis=0, keepdims=True)
    for k in range(0, count, step):
        real = column(pad_v[:, k:k + step].astype(f32)) == 1.0
        same = ccol_v[k:k + step, :spots] == query_c
        itself = (lax.broadcasted_iota(jnp.int32, (step, spots), 0) + k) == (first + lane_spot)
        mask_v[k:k + step, :] = jnp.where(same & (real | itself), 0.0, masked_score)

    def rel_block(q, _):
        diff = code_v[pl.ds(first + q, 1), :classes] - code_v[:, :classes]
        pin_v[q] = mm(bucket_onehot(diff, classes), rel)
        return 0

    lax.fori_loop(0, rows, rel_block, 0, unroll=short)

    arrive(WHA, WHB, WHO, WP, PB)
    wha_v[...] = (wha_v[...].astype(f32) * 0.5).astype(bf16)
    down = who_v[...].astype(f32)
    who_v[...] = (down - jnp.mean(down, axis=-1, keepdims=True)).astype(bf16)
    bins = wp_v.shape[0]
    bias_col = column(pb_v[...])
    even = jnp.full((8, width), 1.0 / width, bf16)
    centers = (lax.broadcasted_iota(jnp.int32, (bins, 1), 0).astype(f32) + 0.5) * (32.0 / bins)
    arrive(WV, WO, WMB, WMA)
    wab_v[:, :width] = wmb_v[...]
    wab_v[:, width:] = wma_v[...]
    wab_sum = mm(jnp.ones((rows, inner), bf16), wab_v[...])

    pair_r[me] = pair_v[pl.ds(first, rows)]

    def take_single(k):
        if k == 0:
            if pairs > 1:
                landed = norm_r.at[pl.ds(0, pairs - 1)]
                pltpu.make_async_copy(landed, landed, recv_sem.at[0, 0]).wait()
            pltpu.make_async_copy(norm_s, norm_s, recv_sem.at[5, 0]).wait()
        else:
            half = norm_r.at[pl.ds(groups[k] * pairs, pairs), side]
            pltpu.make_async_copy(half, half, recv_sem.at[0, k]).wait()
            remote(half, half, 4, k, partner)

    send_pair_either(3, 2, 0, size)
    send_pair(1)
    send_pair(0)
    send_pair_either(2, 3, 0, size * 2 // 4)
    for k in range(parts):
        take_single(k)
    for k in range(1, parts):
        half = norm_r.at[pl.ds(0, pairs), 0]
        pltpu.make_async_copy(half, half, recv_sem.at[4, k]).wait()
    every = norm_r[...].astype(f32).reshape(count, inner).astype(bf16)
    score_v[...] = mm(every, toward) + mask_v[...]
    for k in range(parts):
        take(bias_r, recv_sem.at[1], k)
    values = mm(every, wv_v[...]).astype(bf16)
    scores = score_v[...] + bias_r[...].astype(f32).reshape(count, spots)
    expo = jnp.exp(scores - jnp.max(scores, axis=0, keepdims=True))
    weights = (expo * (1.0 / jnp.sum(expo, axis=0, keepdims=True))).astype(bf16)
    mixed_heads = mm_tn(weights, values)
    attended = mixed_heads[:rows, :]
    for h in range(1, heads):
        attended = jnp.where(head_of == h, mixed_heads[h * rows:(h + 1) * rows, :], attended)
    refined = (mine + mm((gating * attended).astype(bf16), wo_v[...])).astype(bf16)
    raw = mm(refined, wab_v[...])
    exact = refined.astype(f32)
    away = exact - center
    shift = jnp.mean(away, axis=-1, keepdims=True)
    spread = jnp.maximum(jnp.mean(away * away, axis=-1, keepdims=True) - shift * shift, 0.0)
    middle = center + shift
    scale = lax.rsqrt(spread + epsilon)
    factors = ((raw - middle * wab_sum) * scale).astype(bf16)
    factor_b = factors[:, :width]
    b_s[...] = factor_b
    a_v[...] = factors[:, width:].astype(f32)
    b_r[me] = factor_b
    refined_ref[...] = refined

    for k in reversed(range(parts)):
        each_peer(k, lambda peer: remote(b_s, b_r.at[me], 3, k, peer))
    send_pair_either(2, 3, size * 2 // 4, size)

    per = step // sub
    lane_part = lax.broadcasted_iota(jnp.int32, (rows, step), 1) // sub
    row_part = lax.broadcasted_iota(jnp.int32, (rows, step), 0) % per
    row_block = lax.broadcasted_iota(jnp.int32, (rows, step), 0) // per
    block = rows * sub

    def place_of(k, off):
        return pl.multiple_of(groups[k] * span + off, sub)

    def mix(k, off):
        at = place_of(k, off)
        near = pl.ds(at // rows, sub // rows)
        factor = b_r[near].astype(f32).reshape(sub, width)
        for q in range(rows):
            flat = (pin_v[q, pl.ds(at, sub), :] + pair_r[near, q].astype(f32).reshape(sub, width)
                    + a_v[q:q + 1, :] * factor)
            row = k * block + q * sub
            center = flat - jnp.mean(flat, axis=-1, keepdims=True)
            spread = jnp.mean(center * center, axis=-1, keepdims=True)
            flat_v[row:row + sub, :] = center
            x_v[row:row + sub, :] = center.astype(bf16)
            scale_v[row:row + sub, :] = jnp.broadcast_to(lax.rsqrt(spread + epsilon), (sub, 128))

    def expand(ks):
        cut = 256
        for c in range(0, wha_v.shape[1], cut):
            wa = wha_v[:, c:c + cut]
            wb = whb_v[:, c:c + cut]
            for k in ks:
                for r in range(k * block, (k + 1) * block, step):
                    x = x_v[r:r + step, :]
                    scale = jnp.tile(scale_v[r:r + step, :], (1, cut // 128))
                    half = mm(x, wa) * scale
                    up = mm(x, wb) * scale
                    hid_v[r:r + step, c:c + cut] = ((half + half * jnp.tanh(half)) * up).astype(bf16)

    def reduce(k):
        for r in range(k * block, (k + 1) * block, step):
            center = flat_v[r:r + step, :] + mm(hid_v[r:r + step, :], who_v[...])
            x_v[r:r + step, :] = center.astype(bf16)
            square_v[r:r + step, :] = (center * center).astype(bf16)

    def grade(k, off):
        found = jnp.zeros((rows, step), f32)
        for v in range(rows // per):
            r = k * block + v * step
            spread = mm_nt(even, square_v[r:r + step, :])[0:1]
            logits = mm_nt(wp_v[...], x_v[r:r + step, :]) * lax.rsqrt(spread + epsilon) + bias_col
            expo = jnp.exp(logits - jnp.max(logits, axis=0, keepdims=True))
            value = (jnp.sum(expo * centers, axis=0, keepdims=True)
                     / jnp.sum(expo, axis=0, keepdims=True))
            found = jnp.where(row_block == v, value, found)
        spread = found
        for u in range(1, per):
            spread = jnp.where((lane_part + per - row_part) % per == u,
                               pltpu.roll(found, u * sub, 1), spread)
        at = place_of(k, off)
        where = pl.ds(pl.multiple_of(at // step * step, step), step)
        errors_ref[:, where] = jnp.where(
            lane_part == (at // sub) % per, spread, errors_ref[:, where])

    def ready(k):
        take(pair_r, recv_sem.at[2], k)
        take(b_r, recv_sem.at[3], k)

    errors_ref[...] = jnp.zeros_like(errors_ref)
    if short and parts == 4:
        take(b_r, recv_sem.at[3], 0)
        take(pair_r, recv_sem.at[2], 0)
        take(b_r, recv_sem.at[3], 1)
        take(pair_r, recv_sem.at[2], 1)
        mix(0, 0)
        mix(1, 0)
        expand((0,1,))
        reduce(0)
        reduce(1)
        take(b_r, recv_sem.at[3], 2)
        take(pair_r, recv_sem.at[2], 2)
        mix(2, 0)
        grade(0, 0)
        grade(1, 0)
        expand((2,))
        take(b_r, recv_sem.at[3], 3)
        take(pair_r, recv_sem.at[2], 3)
        mix(3, 0)
        reduce(2)
        expand((3,))
        grade(2, 0)
        reduce(3)
        grade(3, 0)
    else:
        for k in range(parts):
            ready(k)

        def more(c, _):
            for k in range(parts):
                mix(k, c * sub)
                expand((k,))
                reduce(k)
                grade(k, c * sub)
            return 0

        lax.fori_loop(0, span // sub, more, 0)

    def sent(buf, i, amount):
        out = buf.at[pl.ds(0, amount)]
        pltpu.make_async_copy(out, out, send_sem.at[i]).wait()

    sent(bias_r, 1, n - 1)
    sent(pair_r, 2, n - 1)
    sent(b_r, 3, n - 1)
    pltpu.make_async_copy(norm_s, norm_s, send_sem.at[5]).wait()
    if n > 2:
        sent(norm_r, 0, (size - 2 + (parts - 1) * pairs) // 2)
    if parts > 1:
        sent(norm_r, 4, (parts - 1) * pairs // 2)


def place(refined_v, errors_v, refined_h, errors_h, sem):
    copies = (
        pltpu.make_async_copy(refined_v, refined_h, sem.at[0]),
        pltpu.make_async_copy(errors_v, errors_h, sem.at[1]),
    )
    for copy in copies:
        copy.start()
    for copy in copies:
        copy.wait()


def on_device(n, pair_repr, single_repr, residue_index, chain_index, complex_index, pad_mask,
              w_query, w_key, w_value, w_gate, w_out, w_bias, rel_table, w_mix_a, w_mix_b,
              w_hidden_a, w_hidden_b, w_hidden_out, w_pae, pae_bias):
    count, rows, width = pair_repr.shape
    inner = single_repr.shape[1]
    heads = w_bias.shape[1]
    hidden = w_hidden_a.shape[1]
    args = (pair_repr, single_repr, residue_index[None], chain_index[None], complex_index[None],
            pad_mask[None], w_query, w_key, w_value, w_gate, w_out, w_bias.T, rel_table,
            w_mix_a, w_mix_b, w_hidden_a, w_hidden_b, w_hidden_out, w_pae.T, pae_bias[None])
    spots = rows * heads
    step = min(count, 128)
    scratch = [pltpu.VMEM(a.shape, a.dtype) for a in args] + [
        pltpu.VMEM((count, 128), f32),
        pltpu.VMEM((count, 128), f32),
        pltpu.VMEM((count, spots), f32),
        pltpu.VMEM((n, rows, spots), bf16),
        pltpu.VMEM((n, rows, spots), bf16),
        pltpu.VMEM((rows, inner), bf16),
        pltpu.VMEM((n // 2, 2, rows, inner), bf16),
        pltpu.VMEM((n, rows, rows, width), bf16),
        pltpu.VMEM((rows, width), bf16),
        pltpu.VMEM((n, rows, width), bf16),
        pltpu.VMEM((rows, width), f32),
        pltpu.VMEM((rows, count, width), f32),
        pltpu.VMEM((rows * step, width), f32),
        pltpu.VMEM((rows * step, width), bf16),
        pltpu.VMEM((rows * step, hidden), bf16),
        pltpu.VMEM((inner, 2 * width), bf16),
        pltpu.VMEM((rows * step, 128), f32),
        pltpu.VMEM((rows * step, width), bf16),
        pltpu.VMEM((count, spots), f32),
        pltpu.SemaphoreType.DMA((len(args),)),
        pltpu.SemaphoreType.DMA((6,)),
        pltpu.SemaphoreType.DMA((6, 4)),
    ]
    refined, errors = pl.pallas_call(
        functools.partial(kernel, n, heads),
        out_shape=(pltpu.VMEM((rows, inner), bf16), pltpu.VMEM((rows, count), f32)),
        in_specs=[pl.BlockSpec(memory_space=pltpu.HBM)] * len(args),
        out_specs=[pl.BlockSpec(memory_space=pltpu.VMEM)] * 2,
        scratch_shapes=scratch,
        compiler_params=pltpu.CompilerParams(
            collective_id=0, has_side_effects=True, vmem_limit_bytes=40 * 1024 * 1024),
        name="confidence",
    )(*[pltpu.with_memory_space_constraint(a, pltpu.HBM) for a in args])
    return pl.pallas_call(
        place,
        out_shape=(
            jax.ShapeDtypeStruct((rows, inner), bf16),
            jax.ShapeDtypeStruct((rows, count), f32),
        ),
        in_specs=[pl.BlockSpec(memory_space=pltpu.VMEM)] * 2,
        out_specs=[pl.BlockSpec(memory_space=pltpu.HBM)] * 2,
        scratch_shapes=[pltpu.SemaphoreType.DMA((2,))],
        compiler_params=pltpu.CompilerParams(vmem_limit_bytes=1024 * 1024),
        name="place",
    )(refined, errors)


def solution(mesh):
    placed = (
        P("groups", "rows", None),
        P(("groups", "rows"), None),
        P("groups"),
        P("groups"),
        P("groups"),
        P("groups"),
    ) + (P(),) * 14
    return jax.shard_map(
        functools.partial(on_device, mesh.shape["rows"]),
        mesh=mesh,
        in_specs=placed,
        out_specs=(P(("groups", "rows"), None), P(("groups", "rows"), None)),
        check_vma=False,
    )
```

```python
import functools
import math

import jax
import jax.numpy as jnp
from jax import lax
from jax.experimental import pallas as pl
from jax.experimental.pallas import tpu as pltpu
from jax.sharding import PartitionSpec as P

epsilon = 1e-05
masked_score = -1e30
chain_step = 65536.0
f32 = jnp.float32
bf16 = jnp.bfloat16


def norm_rows(values):
    center = values - jnp.mean(values, axis=-1, keepdims=True)
    spread = jnp.mean(center * center, axis=-1, keepdims=True)
    return center * lax.rsqrt(spread + epsilon)


def mm(a, b):
    return jnp.dot(a, b, preferred_element_type=f32)


def mm_nt(a, b):
    return lax.dot_general(a, b, (((1,), (1,)), ((), ())), preferred_element_type=f32)


def mm_tn(a, b):
    return lax.dot_general(a, b, (((0,), (0,)), ((), ())), preferred_element_type=f32)


def column(row):
    m = row.shape[1]
    pick = lax.broadcasted_iota(jnp.int32, (m, m), 0) == lax.broadcasted_iota(jnp.int32, (m, m), 1)
    return jnp.sum(jnp.where(pick, row, 0.0), axis=1, keepdims=True)


def bucket_onehot(diff, classes):
    reach = (classes - 2) // 2
    same = jnp.abs(diff) < 0.5 * chain_step
    bucket = jnp.where(same, jnp.clip(diff, -reach, reach) + reach, 2.0 * reach + 1.0)
    lanes = lax.broadcasted_iota(jnp.int32, bucket.shape, bucket.ndim - 1).astype(f32)
    return jnp.where(bucket == lanes, 1.0, 0.0).astype(bf16)


def kernel(
    n,
    heads,
    pair_h, single_h, res_h, chain_h, complex_h, pad_h,
    wq_h, wk_h, wv_h, wg_h, wo_h, wb_h, rel_h, wma_h, wmb_h, wha_h, whb_h, who_h, wp_h, pb_h,
    refined_ref, errors_ref,
    pair_v, single_v, res_v, chain_v, complex_v, pad_v,
    wq_v, wk_v, wv_v, wg_v, wo_v, wb_v, rel_v, wma_v, wmb_v, wha_v, whb_v, who_v, wp_v, pb_v,
    code_v, ccol_v, mask_v, bias_s, bias_r, norm_s, norm_r, pair_r, b_s, b_r, a_v, pin_v,
    flat_v, x_v, hid_v, wab_v, scale_v, square_v, score_v,
    two_v, gate_v, toward_v, sum_v, a_s, a_r, refined_s, refined_r,
    local_sem, send_sem, recv_sem,
):
    me = lax.axis_index("rows")
    count, rows, width = pair_h.shape
    classes = rel_h.shape[0]
    inner = single_h.shape[1]
    head_size = inner // heads
    spots = rows * heads
    first = pl.multiple_of(me * rows, rows)
    step = min(count, 128)
    short = count == step
    sub = 32

    hbm = (pair_h, single_h, res_h, chain_h, complex_h, pad_h, wq_h, wk_h, wv_h, wg_h, wo_h,
           wb_h, rel_h, wma_h, wmb_h, wha_h, whb_h, who_h, wp_h, pb_h)
    vmem = (pair_v, single_v, res_v, chain_v, complex_v, pad_v, wq_v, wk_v, wv_v, wg_v, wo_v,
            wb_v, rel_v, wma_v, wmb_v, wha_v, whb_v, who_v, wp_v, pb_v)
    (PAIR, SINGLE, RES, CHAIN, COMPLEX, PAD, WQ, WK, WV, WG, WO, WB, REL, WMA, WMB, WHA, WHB,
     WHO, WP, PB) = range(len(hbm))
    loads = [pltpu.make_async_copy(h, v, local_sem.at[i]) for i, (h, v) in enumerate(zip(hbm, vmem))]

    def arrive(*which):
        for i in which:
            loads[i].wait()

    parts = 4 if n % 4 == 0 else 1
    size = n // parts
    mine_at = me % size
    group = me // size
    low = group % 2
    groups = (group, group + 1 - 2 * low, group + 2 - 4 * (group // 2), 3 - group)[:parts]
    span = size * rows

    def each_peer(k, visit):
        base = groups[k] * size

        def body(s, _):
            visit(base + (mine_at + s) % size)
            return 0

        if short:
            for s in range(1 if k == 0 else 0, size):
                body(s, 0)
        else:
            lax.fori_loop(1 if k == 0 else 0, size, body, 0)

    def take(buf, sems, k):
        landed = buf.at[pl.ds(0, size - (1 if k == 0 else 0))]
        pltpu.make_async_copy(landed, landed, sems.at[k]).wait()

    barrier = pltpu.get_barrier_semaphore()
    for k in reversed(range(parts)):
        each_peer(k, lambda peer: pl.semaphore_signal(
            barrier, inc=1, device_id={"rows": peer}, device_id_type=pl.DeviceIdType.MESH))
    for i in (RES, CHAIN, SINGLE, REL, WB, PAIR, COMPLEX, PAD, WQ, WG, WK, WV, WO, WMB, WMA, WHA, WHB, WHO, WP, PB):
        loads[i].start()

    arrive(RES, CHAIN)
    for k in range(0, count, step):
        code = chain_v[:, k:k + step].astype(f32) * chain_step + res_v[:, k:k + step].astype(f32)
        code_v[k:k + step, :] = jnp.broadcast_to(column(code), (step, 128))

    arrive(SINGLE)
    mine = single_v[...].astype(f32)
    center = jnp.mean(mine, axis=-1, keepdims=True)
    normed = norm_rows(mine).astype(bf16)
    norm_s[...] = normed
    norm_r[me] = normed
    two_v[me % 2] = single_v[...]

    arrive(REL, WB, PAIR)
    rel = rel_v[...]
    tile_h = jnp.where(
        lax.broadcasted_iota(jnp.int32, (heads, spots), 1) // rows
        == lax.broadcasted_iota(jnp.int32, (heads, spots), 0), 1.0, 0.0).astype(bf16)
    w_tiled = mm_tn(wb_v[...], tile_h).astype(bf16)
    code_keys = code_v[pl.ds(first, rows), :classes]

    def bias_block(j, _):
        at = pl.multiple_of(j * step, step)
        code_i = code_v[pl.ds(at, step), :classes]
        diff = code_i[:, None, :] - code_keys[None, :, :]
        hot = bucket_onehot(diff.reshape(step * rows, classes), classes)
        cells = mm(hot, rel) + pair_v[pl.ds(at, step)].astype(f32).reshape(step * rows, width)
        out = mm(norm_rows(cells).astype(bf16), w_tiled)
        out = out.reshape(step // rows, rows, rows, spots)
        lane_q = lax.broadcasted_iota(jnp.int32, (1, 1, spots), 2) % rows
        total = jnp.where(lane_q == 0, out[:, 0], 0.0)
        for q in range(1, rows):
            total = jnp.where(lane_q == q, out[:, q], total)
        bias_s[pl.ds(pl.multiple_of(j * (step // rows), step // rows), step // rows)] = total.astype(bf16)
        return 0

    lax.fori_loop(0, count // step, bias_block, 0, unroll=short)
    bias_r[me] = bias_s[pl.ds(me - me % 2, 2)]

    pl.semaphore_wait(barrier, n - 1)

    def remote(src, dst, i, at, peer):
        pltpu.make_async_remote_copy(
            src_ref=src, dst_ref=dst, send_sem=send_sem.at[i], recv_sem=recv_sem.at[at],
            device_id={"rows": peer}, device_id_type=pl.DeviceIdType.MESH).start()

    side = me % 2
    chip = me - side
    partner = me + 1 - 2 * side
    pairs = size // 2

    def each_chip(k, visit):
        def body(s, _):
            visit(groups[k] * size + 2 * ((mine_at // 2 + s) % pairs))
            return 0

        if short:
            for s in range(1 if k == 0 else 0, pairs):
                body(s, 0)
        else:
            lax.fori_loop(1 if k == 0 else 0, pairs, body, 0)

    @pl.when(side == 0)
    def _():
        remote(norm_s, norm_r.at[me], 4, (4, 0), partner)
        remote(single_v, two_v.at[0], 5, (4, 1), partner)

    for k in reversed(range(parts)):
        each_chip(k, lambda to: remote(norm_s, norm_r.at[me], 0, (0, k), to + 1))
    for k in reversed(range(parts)):
        each_chip(k, lambda to: remote(bias_s.at[pl.ds(to, 2)], bias_r.at[me], 1, (1, k), to + 1))

    @pl.when(side == 0)
    def _():
        remote(bias_s.at[pl.ds(chip, 2)], bias_r.at[me], 6, (4, 2), partner)

    def send_pair(k):
        each_peer(k, lambda peer: remote(
            pair_v.at[pl.ds(peer * rows, rows)], pair_r.at[me], 2, (2, k), peer))

    def send_pair_either(edge, middle, low, high):
        inside = group * (3 - group) // 2
        k = edge + (middle - edge) * inside
        base = (groups[edge] + (groups[middle] - groups[edge]) * inside) * size

        def body(s, _):
            peer = base + (mine_at + s) % size
            remote(pair_v.at[pl.ds(peer * rows, rows)], pair_r.at[me], 2, (2, k), peer)
            return 0

        if short:
            for s in range(low, high):
                body(s, 0)
        else:
            lax.fori_loop(low, high, body, 0)

    def landed(buf, at):
        pltpu.make_async_copy(buf, buf, recv_sem.at[at]).wait()

    arrive(COMPLEX, PAD, WQ, WG, WK)
    head_of = lax.broadcasted_iota(jnp.int32, (rows, inner), 1) // head_size

    @pl.when(side == 1)
    def _():
        landed(norm_s, (4, 0))
        both = norm_r[pl.ds(chip, 2)].astype(f32).reshape(2 * rows, inner).astype(bf16)
        queries = mm(both, wq_v[...]).astype(bf16).astype(f32)
        gate_v[...] = jax.nn.sigmoid(mm(both, wg_v[...]))
        q_wide = jnp.concatenate(
            [jnp.where(head_of == h, queries[c * rows:(c + 1) * rows], 0.0)
             for c in (0, 1) for h in range(heads)], axis=0).astype(bf16)
        toward_v[...] = (mm_nt(wk_v[...], q_wide) / math.sqrt(head_size)).astype(bf16)
        lane_spot = lax.broadcasted_iota(jnp.int32, (step, spots), 1) % rows
        for k in range(0, count, step):
            ccol_v[k:k + step, :] = jnp.broadcast_to(
                column(complex_v[:, k:k + step].astype(f32)), (step, 128))
        lane_row = lax.broadcasted_iota(jnp.int32, (rows, spots), 1) % rows
        pick = lane_row == lax.broadcasted_iota(jnp.int32, (rows, spots), 0)
        for c in (0, 1):
            start = (chip + c) * rows
            mine_c = ccol_v[pl.ds(pl.multiple_of(start, rows), rows), 0:1]
            query_c = jnp.sum(jnp.where(pick, mine_c, 0.0), axis=0, keepdims=True)
            for k in range(0, count, step):
                real = column(pad_v[:, k:k + step].astype(f32)) == 1.0
                same = ccol_v[k:k + step, :spots] == query_c
                itself = (lax.broadcasted_iota(jnp.int32, (step, spots), 0) + k) == (start + lane_spot)
                mask_v[k:k + step, c * spots:(c + 1) * spots] = jnp.where(
                    same & (real | itself), 0.0, masked_score)

    def rel_block(q, _):
        diff = code_v[pl.ds(first + q, 1), :classes] - code_v[:, :classes]
        pin_v[q] = mm(bucket_onehot(diff, classes), rel)
        return 0

    lax.fori_loop(0, rows, rel_block, 0, unroll=short)

    arrive(WHA, WHB, WHO, WP, PB)
    wha_v[...] = (wha_v[...].astype(f32) * 0.5).astype(bf16)
    down = who_v[...].astype(f32)
    who_v[...] = (down - jnp.mean(down, axis=-1, keepdims=True)).astype(bf16)
    bins = wp_v.shape[0]
    bias_col = column(pb_v[...])
    even = jnp.full((8, width), 1.0 / width, bf16)
    centers = (lax.broadcasted_iota(jnp.int32, (bins, 1), 0).astype(f32) + 0.5) * (32.0 / bins)
    arrive(WV, WO, WMB, WMA)
    wab_v[:, :width] = wmb_v[...]
    wab_v[:, width:] = wma_v[...]
    sum_v[...] = mm(jnp.ones((rows, inner), bf16), wab_v[...])

    pair_r[me] = pair_v[pl.ds(first, rows)]

    send_pair_either(3, 2, 0, size)
    send_pair(1)
    send_pair(0)
    send_pair_either(2, 3, 0, size * 2 // 4)

    @pl.when(side == 1)
    def _():
        for k in range(parts):
            landed(norm_r.at[pl.ds(0, size - (2 if k == 0 else 0))], (0, k))
        every = norm_r[...].astype(f32).reshape(count, inner).astype(bf16)
        score_v[...] = mm(every, toward_v[...]) + mask_v[...]
        landed(two_v.at[0], (4, 1))
        landed(bias_s.at[pl.ds(0, 2)], (4, 2))
        for k in range(parts):
            landed(bias_r.at[pl.ds(0, size - (2 if k == 0 else 0))], (1, k))
        values = mm(every, wv_v[...]).astype(bf16)
        attended = []
        for c in (0, 1):
            scores = (score_v[:, c * spots:(c + 1) * spots]
                      + bias_r[:, c].astype(f32).reshape(count, spots))
            expo = jnp.exp(scores - jnp.max(scores, axis=0, keepdims=True))
            weights = (expo * (1.0 / jnp.sum(expo, axis=0, keepdims=True))).astype(bf16)
            mixed_heads = mm_tn(weights, values)
            found = mixed_heads[:rows, :]
            for h in range(1, heads):
                found = jnp.where(head_of == h, mixed_heads[h * rows:(h + 1) * rows, :], found)
            attended.append(found)
        attended = jnp.concatenate(attended, axis=0)
        before = two_v[...].astype(f32).reshape(2 * rows, inner)
        center = jnp.mean(before, axis=-1, keepdims=True)
        refined = (before + mm((gate_v[...] * attended).astype(bf16), wo_v[...])).astype(bf16)
        raw = mm(refined, wab_v[...])
        away = refined.astype(f32) - center
        shift = jnp.mean(away, axis=-1, keepdims=True)
        spread = jnp.maximum(jnp.mean(away * away, axis=-1, keepdims=True) - shift * shift, 0.0)
        factors = ((raw - (center + shift) * sum_v[0:1, :]) * lax.rsqrt(spread + epsilon))
        factors = factors.astype(bf16).astype(f32)
        for c in (0, 1):
            b_s[c] = factors[c * rows:(c + 1) * rows, :width].astype(bf16)
            b_r[chip + c] = factors[c * rows:(c + 1) * rows, :width].astype(bf16)
        a_s[...] = factors[:rows, width:].astype(bf16)
        refined_s[...] = refined.astype(f32)[:rows].astype(bf16)
        for k in reversed(range(parts)):
            each_chip(k, lambda to: remote(b_s, b_r.at[pl.ds(chip, 2)], 7, (3, k), to))
            each_chip(k, lambda to: remote(b_s, b_r.at[pl.ds(chip, 2)], 3, (3, k), to + 1))
        remote(b_s, b_r.at[pl.ds(chip, 2)], 8, (5, 0), partner)
        remote(a_s, a_r, 9, (5, 1), partner)
        remote(refined_s, refined_r, 10, (5, 2), partner)
        a_v[...] = factors[rows:, width:]
        refined_ref[...] = refined.astype(f32)[rows:].astype(bf16)

    @pl.when(side == 0)
    def _():
        landed(b_s, (5, 0))
        landed(a_s, (5, 1))
        landed(refined_s, (5, 2))
        a_v[...] = a_r[...].astype(f32)
        refined_ref[...] = refined_r[...]

    send_pair_either(2, 3, size * 2 // 4, size)

    per = step // sub
    lane_part = lax.broadcasted_iota(jnp.int32, (rows, step), 1) // sub
    row_part = lax.broadcasted_iota(jnp.int32, (rows, step), 0) % per
    row_block = lax.broadcasted_iota(jnp.int32, (rows, step), 0) // per
    block = rows * sub

    def place_of(k, off):
        return pl.multiple_of(groups[k] * span + off, sub)

    def mix(k, off):
        at = place_of(k, off)
        near = pl.ds(at // rows, sub // rows)
        factor = b_r[near].astype(f32).reshape(sub, width)
        for q in range(rows):
            flat = (pin_v[q, pl.ds(at, sub), :] + pair_r[near, q].astype(f32).reshape(sub, width)
                    + a_v[q:q + 1, :] * factor)
            row = k * block + q * sub
            center = flat - jnp.mean(flat, axis=-1, keepdims=True)
            spread = jnp.mean(center * center, axis=-1, keepdims=True)
            flat_v[row:row + sub, :] = center
            x_v[row:row + sub, :] = center.astype(bf16)
            scale_v[row:row + sub, :] = jnp.broadcast_to(lax.rsqrt(spread + epsilon), (sub, 128))

    def expand(ks):
        cut = 256
        for c in range(0, wha_v.shape[1], cut):
            wa = wha_v[:, c:c + cut]
            wb = whb_v[:, c:c + cut]
            for k in ks:
                for r in range(k * block, (k + 1) * block, step):
                    x = x_v[r:r + step, :]
                    scale = jnp.tile(scale_v[r:r + step, :], (1, cut // 128))
                    half = mm(x, wa) * scale
                    up = mm(x, wb) * scale
                    hid_v[r:r + step, c:c + cut] = ((half + half * jnp.tanh(half)) * up).astype(bf16)

    def reduce(k):
        for r in range(k * block, (k + 1) * block, step):
            center = flat_v[r:r + step, :] + mm(hid_v[r:r + step, :], who_v[...])
            x_v[r:r + step, :] = center.astype(bf16)
            square_v[r:r + step, :] = (center * center).astype(bf16)

    def grade(k, off):
        found = jnp.zeros((rows, step), f32)
        for v in range(rows // per):
            r = k * block + v * step
            spread = mm_nt(even, square_v[r:r + step, :])[0:1]
            logits = mm_nt(wp_v[...], x_v[r:r + step, :]) * lax.rsqrt(spread + epsilon) + bias_col
            expo = jnp.exp(logits - jnp.max(logits, axis=0, keepdims=True))
            value = (jnp.sum(expo * centers, axis=0, keepdims=True)
                     / jnp.sum(expo, axis=0, keepdims=True))
            found = jnp.where(row_block == v, value, found)
        spread = found
        for u in range(1, per):
            spread = jnp.where((lane_part + per - row_part) % per == u,
                               pltpu.roll(found, u * sub, 1), spread)
        at = place_of(k, off)
        where = pl.ds(pl.multiple_of(at // step * step, step), step)
        errors_ref[:, where] = jnp.where(
            lane_part == (at // sub) % per, spread, errors_ref[:, where])

    def ready(k):
        take(pair_r, recv_sem.at[2], k)
        landed(b_r.at[pl.ds(0, size - (2 if k == 0 else 0))], (3, k))

    errors_ref[...] = jnp.zeros_like(errors_ref)
    if short and parts == 4:
        landed(b_r.at[pl.ds(0, size - 2)], (3, 0))
        take(pair_r, recv_sem.at[2], 0)
        landed(b_r.at[pl.ds(0, size)], (3, 1))
        take(pair_r, recv_sem.at[2], 1)
        mix(0, 0)
        mix(1, 0)
        expand((0,1,))
        reduce(0)
        reduce(1)
        landed(b_r.at[pl.ds(0, size)], (3, 2))
        take(pair_r, recv_sem.at[2], 2)
        mix(2, 0)
        grade(0, 0)
        grade(1, 0)
        expand((2,))
        landed(b_r.at[pl.ds(0, size)], (3, 3))
        take(pair_r, recv_sem.at[2], 3)
        mix(3, 0)
        reduce(2)
        expand((3,))
        grade(2, 0)
        reduce(3)
        grade(3, 0)
    else:
        for k in range(parts):
            ready(k)

        def more(c, _):
            for k in range(parts):
                mix(k, c * sub)
                expand((k,))
                reduce(k)
                grade(k, c * sub)
            return 0

        lax.fori_loop(0, span // sub, more, 0)

    def sent(buf, i, amount):
        out = buf.at[pl.ds(0, amount)]
        pltpu.make_async_copy(out, out, send_sem.at[i]).wait()

    sent(norm_r, 0, n // 2 - 1)
    sent(bias_r, 1, n // 2 - 1)
    sent(pair_r, 2, n - 1)

    @pl.when(side == 0)
    def _():
        pltpu.make_async_copy(norm_s, norm_s, send_sem.at[4]).wait()
        pltpu.make_async_copy(single_v, single_v, send_sem.at[5]).wait()
        sent(bias_s, 6, 2)

    @pl.when(side == 1)
    def _():
        sent(b_r, 3, n - 2)
        sent(b_r, 7, n - 2)
        pltpu.make_async_copy(b_s, b_s, send_sem.at[8]).wait()
        pltpu.make_async_copy(a_s, a_s, send_sem.at[9]).wait()
        pltpu.make_async_copy(refined_s, refined_s, send_sem.at[10]).wait()


def place(refined_v, errors_v, refined_h, errors_h, sem):
    copies = (
        pltpu.make_async_copy(refined_v, refined_h, sem.at[0]),
        pltpu.make_async_copy(errors_v, errors_h, sem.at[1]),
    )
    for copy in copies:
        copy.start()
    for copy in copies:
        copy.wait()


def on_device(n, pair_repr, single_repr, residue_index, chain_index, complex_index, pad_mask,
              w_query, w_key, w_value, w_gate, w_out, w_bias, rel_table, w_mix_a, w_mix_b,
              w_hidden_a, w_hidden_b, w_hidden_out, w_pae, pae_bias):
    count, rows, width = pair_repr.shape
    inner = single_repr.shape[1]
    heads = w_bias.shape[1]
    hidden = w_hidden_a.shape[1]
    args = (pair_repr, single_repr, residue_index[None], chain_index[None], complex_index[None],
            pad_mask[None], w_query, w_key, w_value, w_gate, w_out, w_bias.T, rel_table,
            w_mix_a, w_mix_b, w_hidden_a, w_hidden_b, w_hidden_out, w_pae.T, pae_bias[None])
    spots = rows * heads
    step = min(count, 128)
    scratch = [pltpu.VMEM(a.shape, a.dtype) for a in args] + [
        pltpu.VMEM((count, 128), f32),
        pltpu.VMEM((count, 128), f32),
        pltpu.VMEM((count, 2 * spots), f32),
        pltpu.VMEM((n, rows, spots), bf16),
        pltpu.VMEM((n, 2, rows, spots), bf16),
        pltpu.VMEM((rows, inner), bf16),
        pltpu.VMEM((n, rows, inner), bf16),
        pltpu.VMEM((n, rows, rows, width), bf16),
        pltpu.VMEM((2, rows, width), bf16),
        pltpu.VMEM((n, rows, width), bf16),
        pltpu.VMEM((rows, width), f32),
        pltpu.VMEM((rows, count, width), f32),
        pltpu.VMEM((rows * step, width), f32),
        pltpu.VMEM((rows * step, width), bf16),
        pltpu.VMEM((rows * step, hidden), bf16),
        pltpu.VMEM((inner, 2 * width), bf16),
        pltpu.VMEM((rows * step, 128), f32),
        pltpu.VMEM((rows * step, width), bf16),
        pltpu.VMEM((count, 2 * spots), f32),
        pltpu.VMEM((2, rows, inner), bf16),
        pltpu.VMEM((2 * rows, inner), f32),
        pltpu.VMEM((inner, 2 * spots), bf16),
        pltpu.VMEM((rows, 2 * width), f32),
        pltpu.VMEM((rows, width), bf16),
        pltpu.VMEM((rows, width), bf16),
        pltpu.VMEM((rows, inner), bf16),
        pltpu.VMEM((rows, inner), bf16),
        pltpu.SemaphoreType.DMA((len(args),)),
        pltpu.SemaphoreType.DMA((11,)),
        pltpu.SemaphoreType.DMA((6, 4)),
    ]
    refined, errors = pl.pallas_call(
        functools.partial(kernel, n, heads),
        out_shape=(pltpu.VMEM((rows, inner), bf16), pltpu.VMEM((rows, count), f32)),
        in_specs=[pl.BlockSpec(memory_space=pltpu.HBM)] * len(args),
        out_specs=[pl.BlockSpec(memory_space=pltpu.VMEM)] * 2,
        scratch_shapes=scratch,
        compiler_params=pltpu.CompilerParams(
            collective_id=0, has_side_effects=True, vmem_limit_bytes=40 * 1024 * 1024),
        name="confidence",
    )(*[pltpu.with_memory_space_constraint(a, pltpu.HBM) for a in args])
    return pl.pallas_call(
        place,
        out_shape=(
            jax.ShapeDtypeStruct((rows, inner), bf16),
            jax.ShapeDtypeStruct((rows, count), f32),
        ),
        in_specs=[pl.BlockSpec(memory_space=pltpu.VMEM)] * 2,
        out_specs=[pl.BlockSpec(memory_space=pltpu.HBM)] * 2,
        scratch_shapes=[pltpu.SemaphoreType.DMA((2,))],
        compiler_params=pltpu.CompilerParams(vmem_limit_bytes=1024 * 1024),
        name="place",
    )(refined, errors)


def solution(mesh):
    placed = (
        P("groups", "rows", None),
        P(("groups", "rows"), None),
        P("groups"),
        P("groups"),
        P("groups"),
        P("groups"),
    ) + (P(),) * 14
    return jax.shard_map(
        functools.partial(on_device, mesh.shape["rows"]),
        mesh=mesh,
        in_specs=placed,
        out_specs=(P(("groups", "rows"), None), P(("groups", "rows"), None)),
        check_vma=False,
    )
```

```python
import functools
import math

import jax
import jax.numpy as jnp
from jax import lax
from jax.experimental import pallas as pl
from jax.experimental.pallas import tpu as pltpu
from jax.sharding import PartitionSpec as P

epsilon = 1e-05
masked_score = -1e30
chain_step = 65536.0
f32 = jnp.float32
bf16 = jnp.bfloat16


def norm_rows(values):
    center = values - jnp.mean(values, axis=-1, keepdims=True)
    spread = jnp.mean(center * center, axis=-1, keepdims=True)
    return center * lax.rsqrt(spread + epsilon)


def mm(a, b):
    return jnp.dot(a, b, preferred_element_type=f32)


def mm_nt(a, b):
    return lax.dot_general(a, b, (((1,), (1,)), ((), ())), preferred_element_type=f32)


def mm_tn(a, b):
    return lax.dot_general(a, b, (((0,), (0,)), ((), ())), preferred_element_type=f32)


def column(row):
    m = row.shape[1]
    pick = lax.broadcasted_iota(jnp.int32, (m, m), 0) == lax.broadcasted_iota(jnp.int32, (m, m), 1)
    return jnp.sum(jnp.where(pick, row, 0.0), axis=1, keepdims=True)


def bucket_onehot(diff, classes):
    reach = (classes - 2) // 2
    same = jnp.abs(diff) < 0.5 * chain_step
    bucket = jnp.where(same, jnp.clip(diff, -reach, reach) + reach, 2.0 * reach + 1.0)
    lanes = lax.broadcasted_iota(jnp.int32, bucket.shape, bucket.ndim - 1).astype(f32)
    return jnp.where(bucket == lanes, 1.0, 0.0).astype(bf16)


def kernel(
    n,
    heads,
    pair_h, single_h, res_h, chain_h, complex_h, pad_h,
    wq_h, wk_h, wv_h, wg_h, wo_h, wb_h, rel_h, wma_h, wmb_h, wha_h, whb_h, who_h, wp_h, pb_h,
    refined_ref, errors_ref,
    pair_v, single_v, res_v, chain_v, complex_v, pad_v,
    wq_v, wk_v, wv_v, wg_v, wo_v, wb_v, rel_v, wma_v, wmb_v, wha_v, whb_v, who_v, wp_v, pb_v,
    code_v, ccol_v, mask_v, bias_s, bias_r, norm_s, norm_r, pair_r, b_s, b_r, a_v, pin_v,
    flat_v, x_v, hid_v, wab_v, scale_v, square_v, score_v,
    two_v, gate_v, toward_v, sum_v, a_s, a_r, refined_s, refined_r,
    local_sem, send_sem, recv_sem,
):
    me = lax.axis_index("rows")
    count, rows, width = pair_h.shape
    classes = rel_h.shape[0]
    inner = single_h.shape[1]
    head_size = inner // heads
    spots = rows * heads
    first = pl.multiple_of(me * rows, rows)
    step = min(count, 128)
    short = count == step
    sub = 32

    hbm = (pair_h, single_h, res_h, chain_h, complex_h, pad_h, wq_h, wk_h, wv_h, wg_h, wo_h,
           wb_h, rel_h, wma_h, wmb_h, wha_h, whb_h, who_h, wp_h, pb_h)
    vmem = (pair_v, single_v, res_v, chain_v, complex_v, pad_v, wq_v, wk_v, wv_v, wg_v, wo_v,
            wb_v, rel_v, wma_v, wmb_v, wha_v, whb_v, who_v, wp_v, pb_v)
    (PAIR, SINGLE, RES, CHAIN, COMPLEX, PAD, WQ, WK, WV, WG, WO, WB, REL, WMA, WMB, WHA, WHB,
     WHO, WP, PB) = range(len(hbm))
    loads = [pltpu.make_async_copy(h, v, local_sem.at[i]) for i, (h, v) in enumerate(zip(hbm, vmem))]

    def arrive(*which):
        for i in which:
            loads[i].wait()

    parts = 4 if n % 4 == 0 else 1
    size = n // parts
    mine_at = me % size
    group = me // size
    low = group % 2
    groups = (group, group + 1 - 2 * low, group + 2 - 4 * (group // 2), 3 - group)[:parts]
    span = size * rows

    def each_peer(k, visit):
        base = groups[k] * size

        def body(s, _):
            visit(base + (mine_at + s) % size)
            return 0

        if short:
            for s in range(1 if k == 0 else 0, size):
                body(s, 0)
        else:
            lax.fori_loop(1 if k == 0 else 0, size, body, 0)

    def take(buf, sems, k):
        landed = buf.at[pl.ds(0, size - (1 if k == 0 else 0))]
        pltpu.make_async_copy(landed, landed, sems.at[k]).wait()

    barrier = pltpu.get_barrier_semaphore()
    for k in reversed(range(parts)):
        each_peer(k, lambda peer: pl.semaphore_signal(
            barrier, inc=1, device_id={"rows": peer}, device_id_type=pl.DeviceIdType.MESH))
    for i in (RES, CHAIN, SINGLE, REL, WB, PAIR, COMPLEX, PAD, WQ, WG, WK, WV, WO, WMB, WMA, WHA, WHB, WHO, WP, PB):
        loads[i].start()

    arrive(RES, CHAIN)
    for k in range(0, count, step):
        code = chain_v[:, k:k + step].astype(f32) * chain_step + res_v[:, k:k + step].astype(f32)
        code_v[k:k + step, :] = jnp.broadcast_to(column(code), (step, 128))

    arrive(SINGLE)
    mine = single_v[...].astype(f32)
    center = jnp.mean(mine, axis=-1, keepdims=True)
    normed = norm_rows(mine).astype(bf16)
    norm_s[...] = normed
    norm_r[me] = normed
    two_v[me % 2] = single_v[...]

    arrive(REL, WB, PAIR)
    rel = rel_v[...]
    tile_h = jnp.where(
        lax.broadcasted_iota(jnp.int32, (heads, spots), 1) // rows
        == lax.broadcasted_iota(jnp.int32, (heads, spots), 0), 1.0, 0.0).astype(bf16)
    w_tiled = mm_tn(wb_v[...], tile_h).astype(bf16)
    code_keys = code_v[pl.ds(first, rows), :classes]

    def bias_block(j, _):
        at = pl.multiple_of(j * step, step)
        code_i = code_v[pl.ds(at, step), :classes]
        diff = code_i[:, None, :] - code_keys[None, :, :]
        hot = bucket_onehot(diff.reshape(step * rows, classes), classes)
        cells = mm(hot, rel) + pair_v[pl.ds(at, step)].astype(f32).reshape(step * rows, width)
        out = mm(norm_rows(cells).astype(bf16), w_tiled)
        out = out.reshape(step // rows, rows, rows, spots)
        lane_q = lax.broadcasted_iota(jnp.int32, (1, 1, spots), 2) % rows
        total = jnp.where(lane_q == 0, out[:, 0], 0.0)
        for q in range(1, rows):
            total = jnp.where(lane_q == q, out[:, q], total)
        bias_s[pl.ds(pl.multiple_of(j * (step // rows), step // rows), step // rows)] = total.astype(bf16)
        return 0

    lax.fori_loop(0, count // step, bias_block, 0, unroll=short)
    bias_r[me] = bias_s[pl.ds(me - me % 2, 2)]

    pl.semaphore_wait(barrier, n - 1)

    def remote(src, dst, i, at, peer):
        pltpu.make_async_remote_copy(
            src_ref=src, dst_ref=dst, send_sem=send_sem.at[i], recv_sem=recv_sem.at[at],
            device_id={"rows": peer}, device_id_type=pl.DeviceIdType.MESH).start()

    side = me % 2
    chip = me - side
    partner = me + 1 - 2 * side
    pairs = size // 2

    def each_chip(k, visit):
        def body(s, _):
            visit(groups[k] * size + 2 * ((mine_at // 2 + s) % pairs))
            return 0

        if short:
            for s in range(1 if k == 0 else 0, pairs):
                body(s, 0)
        else:
            lax.fori_loop(1 if k == 0 else 0, pairs, body, 0)

    @pl.when(side == 0)
    def _():
        remote(norm_s, norm_r.at[me], 4, (4, 0), partner)
        remote(single_v, two_v.at[0], 5, (4, 1), partner)

    for k in reversed(range(parts)):
        each_chip(k, lambda to: remote(norm_s, norm_r.at[me], 0, (0, k), to + 1))
    for k in reversed(range(parts)):
        each_chip(k, lambda to: remote(bias_s.at[pl.ds(to, 2)], bias_r.at[me], 1, (1, k), to + 1))

    @pl.when(side == 0)
    def _():
        remote(bias_s.at[pl.ds(chip, 2)], bias_r.at[me], 6, (4, 2), partner)

    def send_pair(k):
        each_peer(k, lambda peer: remote(
            pair_v.at[pl.ds(peer * rows, rows)], pair_r.at[me], 2, (2, k), peer))

    def send_pair_either(edge, middle, low, high):
        inside = group * (3 - group) // 2
        k = edge + (middle - edge) * inside
        base = (groups[edge] + (groups[middle] - groups[edge]) * inside) * size

        def body(s, _):
            peer = base + (mine_at + s) % size
            remote(pair_v.at[pl.ds(peer * rows, rows)], pair_r.at[me], 2, (2, k), peer)
            return 0

        if short:
            for s in range(low, high):
                body(s, 0)
        else:
            lax.fori_loop(low, high, body, 0)

    def landed(buf, at):
        pltpu.make_async_copy(buf, buf, recv_sem.at[at]).wait()

    arrive(COMPLEX, PAD, WQ, WG, WK)
    head_of = lax.broadcasted_iota(jnp.int32, (rows, inner), 1) // head_size

    @pl.when(side == 1)
    def _():
        landed(norm_s, (4, 0))
        both = norm_r[pl.ds(chip, 2)].astype(f32).reshape(2 * rows, inner).astype(bf16)
        queries = mm(both, wq_v[...]).astype(bf16).astype(f32)
        gate_v[...] = jax.nn.sigmoid(mm(both, wg_v[...]))
        q_wide = jnp.concatenate(
            [jnp.where(head_of == h, queries[c * rows:(c + 1) * rows], 0.0)
             for c in (0, 1) for h in range(heads)], axis=0).astype(bf16)
        toward_v[...] = (mm_nt(wk_v[...], q_wide) / math.sqrt(head_size)).astype(bf16)
        lane_spot = lax.broadcasted_iota(jnp.int32, (step, spots), 1) % rows
        for k in range(0, count, step):
            ccol_v[k:k + step, :] = jnp.broadcast_to(
                column(complex_v[:, k:k + step].astype(f32)), (step, 128))
        lane_row = lax.broadcasted_iota(jnp.int32, (rows, spots), 1) % rows
        pick = lane_row == lax.broadcasted_iota(jnp.int32, (rows, spots), 0)
        for c in (0, 1):
            start = (chip + c) * rows
            mine_c = ccol_v[pl.ds(pl.multiple_of(start, rows), rows), 0:1]
            query_c = jnp.sum(jnp.where(pick, mine_c, 0.0), axis=0, keepdims=True)
            for k in range(0, count, step):
                real = column(pad_v[:, k:k + step].astype(f32)) == 1.0
                same = ccol_v[k:k + step, :spots] == query_c
                itself = (lax.broadcasted_iota(jnp.int32, (step, spots), 0) + k) == (start + lane_spot)
                mask_v[k:k + step, c * spots:(c + 1) * spots] = jnp.where(
                    same & (real | itself), 0.0, masked_score)

    def rel_block(q, _):
        diff = code_v[pl.ds(first + q, 1), :classes] - code_v[:, :classes]
        pin_v[q] = mm(bucket_onehot(diff, classes), rel)
        return 0

    lax.fori_loop(0, rows, rel_block, 0, unroll=short)

    arrive(WHA, WHB, WHO, WP, PB)
    wha_v[...] = (wha_v[...].astype(f32) * 0.5).astype(bf16)
    down = who_v[...].astype(f32)
    who_v[...] = (down - jnp.mean(down, axis=-1, keepdims=True)).astype(bf16)
    bins = wp_v.shape[0]
    bias_col = column(pb_v[...])
    even = jnp.full((8, width), 1.0 / width, bf16)
    centers = (lax.broadcasted_iota(jnp.int32, (bins, 1), 0).astype(f32) + 0.5) * (32.0 / bins)
    arrive(WV, WO, WMB, WMA)
    wab_v[:, :width] = wmb_v[...]
    wab_v[:, width:] = wma_v[...]
    sum_v[...] = mm(jnp.ones((rows, inner), bf16), wab_v[...])

    pair_r[me] = pair_v[pl.ds(first, rows)]

    send_pair_either(3, 2, 0, size)
    send_pair(1)
    send_pair(0)
    send_pair_either(2, 3, 0, size * 1 // 4)

    @pl.when(side == 1)
    def _():
        for k in range(parts):
            landed(norm_r.at[pl.ds(0, size - (2 if k == 0 else 0))], (0, k))
        every = norm_r[...].astype(f32).reshape(count, inner).astype(bf16)
        score_v[...] = mm(every, toward_v[...]) + mask_v[...]
        landed(two_v.at[0], (4, 1))
        landed(bias_s.at[pl.ds(0, 2)], (4, 2))
        for k in range(parts):
            landed(bias_r.at[pl.ds(0, size - (2 if k == 0 else 0))], (1, k))
        values = mm(every, wv_v[...]).astype(bf16)
        attended = []
        for c in (0, 1):
            scores = (score_v[:, c * spots:(c + 1) * spots]
                      + bias_r[:, c].astype(f32).reshape(count, spots))
            expo = jnp.exp(scores - jnp.max(scores, axis=0, keepdims=True))
            weights = (expo * (1.0 / jnp.sum(expo, axis=0, keepdims=True))).astype(bf16)
            mixed_heads = mm_tn(weights, values)
            found = mixed_heads[:rows, :]
            for h in range(1, heads):
                found = jnp.where(head_of == h, mixed_heads[h * rows:(h + 1) * rows, :], found)
            attended.append(found)
        attended = jnp.concatenate(attended, axis=0)
        before = two_v[...].astype(f32).reshape(2 * rows, inner)
        center = jnp.mean(before, axis=-1, keepdims=True)
        refined = (before + mm((gate_v[...] * attended).astype(bf16), wo_v[...])).astype(bf16)
        raw = mm(refined, wab_v[...])
        away = refined.astype(f32) - center
        shift = jnp.mean(away, axis=-1, keepdims=True)
        spread = jnp.maximum(jnp.mean(away * away, axis=-1, keepdims=True) - shift * shift, 0.0)
        factors = ((raw - (center + shift) * sum_v[0:1, :]) * lax.rsqrt(spread + epsilon))
        factors = factors.astype(bf16).astype(f32)
        for c in (0, 1):
            b_s[c] = factors[c * rows:(c + 1) * rows, :width].astype(bf16)
            b_r[chip + c] = factors[c * rows:(c + 1) * rows, :width].astype(bf16)
        a_s[...] = factors[:rows, width:].astype(bf16)
        refined_s[...] = refined.astype(f32)[:rows].astype(bf16)
        for k in reversed(range(parts)):
            each_chip(k, lambda to: remote(b_s, b_r.at[pl.ds(chip, 2)], 7, (3, k), to))
            each_chip(k, lambda to: remote(b_s, b_r.at[pl.ds(chip, 2)], 3, (3, k), to + 1))
        remote(b_s, b_r.at[pl.ds(chip, 2)], 8, (5, 0), partner)
        remote(a_s, a_r, 9, (5, 1), partner)
        remote(refined_s, refined_r, 10, (5, 2), partner)
        a_v[...] = factors[rows:, width:]
        refined_ref[...] = refined.astype(f32)[rows:].astype(bf16)

    @pl.when(side == 0)
    def _():
        landed(b_s, (5, 0))
        landed(a_s, (5, 1))
        landed(refined_s, (5, 2))
        a_v[...] = a_r[...].astype(f32)
        refined_ref[...] = refined_r[...]

    send_pair_either(2, 3, size * 1 // 4, size)

    per = step // sub
    lane_part = lax.broadcasted_iota(jnp.int32, (rows, step), 1) // sub
    row_part = lax.broadcasted_iota(jnp.int32, (rows, step), 0) % per
    row_block = lax.broadcasted_iota(jnp.int32, (rows, step), 0) // per
    block = rows * sub

    def place_of(k, off):
        return pl.multiple_of(groups[k] * span + off, sub)

    def mix(k, off):
        at = place_of(k, off)
        near = pl.ds(at // rows, sub // rows)
        factor = b_r[near].astype(f32).reshape(sub, width)
        for q in range(rows):
            flat = (pin_v[q, pl.ds(at, sub), :] + pair_r[near, q].astype(f32).reshape(sub, width)
                    + a_v[q:q + 1, :] * factor)
            row = k * block + q * sub
            center = flat - jnp.mean(flat, axis=-1, keepdims=True)
            spread = jnp.mean(center * center, axis=-1, keepdims=True)
            flat_v[row:row + sub, :] = center
            x_v[row:row + sub, :] = center.astype(bf16)
            scale_v[row:row + sub, :] = jnp.broadcast_to(lax.rsqrt(spread + epsilon), (sub, 128))

    def expand(ks):
        cut = 256
        for c in range(0, wha_v.shape[1], cut):
            wa = wha_v[:, c:c + cut]
            wb = whb_v[:, c:c + cut]
            for k in ks:
                for r in range(k * block, (k + 1) * block, step):
                    x = x_v[r:r + step, :]
                    scale = jnp.tile(scale_v[r:r + step, :], (1, cut // 128))
                    half = mm(x, wa) * scale
                    up = mm(x, wb) * scale
                    hid_v[r:r + step, c:c + cut] = ((half + half * jnp.tanh(half)) * up).astype(bf16)

    def reduce(k):
        for r in range(k * block, (k + 1) * block, step):
            center = flat_v[r:r + step, :] + mm(hid_v[r:r + step, :], who_v[...])
            x_v[r:r + step, :] = center.astype(bf16)
            square_v[r:r + step, :] = (center * center).astype(bf16)

    def grade(k, off):
        found = jnp.zeros((rows, step), f32)
        for v in range(rows // per):
            r = k * block + v * step
            spread = mm_nt(even, square_v[r:r + step, :])[0:1]
            logits = mm_nt(wp_v[...], x_v[r:r + step, :]) * lax.rsqrt(spread + epsilon) + bias_col
            expo = jnp.exp(logits - jnp.max(logits, axis=0, keepdims=True))
            value = (jnp.sum(expo * centers, axis=0, keepdims=True)
                     / jnp.sum(expo, axis=0, keepdims=True))
            found = jnp.where(row_block == v, value, found)
        spread = found
        for u in range(1, per):
            spread = jnp.where((lane_part + per - row_part) % per == u,
                               pltpu.roll(found, u * sub, 1), spread)
        at = place_of(k, off)
        where = pl.ds(pl.multiple_of(at // step * step, step), step)
        errors_ref[:, where] = jnp.where(
            lane_part == (at // sub) % per, spread, errors_ref[:, where])

    def ready(k):
        take(pair_r, recv_sem.at[2], k)
        landed(b_r.at[pl.ds(0, size - (2 if k == 0 else 0))], (3, k))

    errors_ref[...] = jnp.zeros_like(errors_ref)
    if short and parts == 4:
        landed(b_r.at[pl.ds(0, size - 2)], (3, 0))
        take(pair_r, recv_sem.at[2], 0)
        landed(b_r.at[pl.ds(0, size)], (3, 1))
        take(pair_r, recv_sem.at[2], 1)
        mix(0, 0)
        mix(1, 0)
        expand((0,))
        expand((1,))
        reduce(0)
        reduce(1)
        landed(b_r.at[pl.ds(0, size)], (3, 2))
        take(pair_r, recv_sem.at[2], 2)
        landed(b_r.at[pl.ds(0, size)], (3, 3))
        take(pair_r, recv_sem.at[2], 3)
        mix(2, 0)
        grade(0, 0)
        mix(3, 0)
        expand((2,))
        grade(1, 0)
        expand((3,))
        reduce(2)
        reduce(3)
        grade(2, 0)
        grade(3, 0)
    else:
        for k in range(parts):
            ready(k)

        def more(c, _):
            for k in range(parts):
                mix(k, c * sub)
                expand((k,))
                reduce(k)
                grade(k, c * sub)
            return 0

        lax.fori_loop(0, span // sub, more, 0)

    def sent(buf, i, amount):
        out = buf.at[pl.ds(0, amount)]
        pltpu.make_async_copy(out, out, send_sem.at[i]).wait()

    sent(norm_r, 0, n // 2 - 1)
    sent(bias_r, 1, n // 2 - 1)
    sent(pair_r, 2, n - 1)

    @pl.when(side == 0)
    def _():
        pltpu.make_async_copy(norm_s, norm_s, send_sem.at[4]).wait()
        pltpu.make_async_copy(single_v, single_v, send_sem.at[5]).wait()
        sent(bias_s, 6, 2)

    @pl.when(side == 1)
    def _():
        sent(b_r, 3, n - 2)
        sent(b_r, 7, n - 2)
        pltpu.make_async_copy(b_s, b_s, send_sem.at[8]).wait()
        pltpu.make_async_copy(a_s, a_s, send_sem.at[9]).wait()
        pltpu.make_async_copy(refined_s, refined_s, send_sem.at[10]).wait()


def place(refined_v, errors_v, refined_h, errors_h, sem):
    copies = (
        pltpu.make_async_copy(refined_v, refined_h, sem.at[0]),
        pltpu.make_async_copy(errors_v, errors_h, sem.at[1]),
    )
    for copy in copies:
        copy.start()
    for copy in copies:
        copy.wait()


def on_device(n, pair_repr, single_repr, residue_index, chain_index, complex_index, pad_mask,
              w_query, w_key, w_value, w_gate, w_out, w_bias, rel_table, w_mix_a, w_mix_b,
              w_hidden_a, w_hidden_b, w_hidden_out, w_pae, pae_bias):
    count, rows, width = pair_repr.shape
    inner = single_repr.shape[1]
    heads = w_bias.shape[1]
    hidden = w_hidden_a.shape[1]
    args = (pair_repr, single_repr, residue_index[None], chain_index[None], complex_index[None],
            pad_mask[None], w_query, w_key, w_value, w_gate, w_out, w_bias.T, rel_table,
            w_mix_a, w_mix_b, w_hidden_a, w_hidden_b, w_hidden_out, w_pae.T, pae_bias[None])
    spots = rows * heads
    step = min(count, 128)
    scratch = [pltpu.VMEM(a.shape, a.dtype) for a in args] + [
        pltpu.VMEM((count, 128), f32),
        pltpu.VMEM((count, 128), f32),
        pltpu.VMEM((count, 2 * spots), f32),
        pltpu.VMEM((n, rows, spots), bf16),
        pltpu.VMEM((n, 2, rows, spots), bf16),
        pltpu.VMEM((rows, inner), bf16),
        pltpu.VMEM((n, rows, inner), bf16),
        pltpu.VMEM((n, rows, rows, width), bf16),
        pltpu.VMEM((2, rows, width), bf16),
        pltpu.VMEM((n, rows, width), bf16),
        pltpu.VMEM((rows, width), f32),
        pltpu.VMEM((rows, count, width), f32),
        pltpu.VMEM((rows * step, width), f32),
        pltpu.VMEM((rows * step, width), bf16),
        pltpu.VMEM((rows * step, hidden), bf16),
        pltpu.VMEM((inner, 2 * width), bf16),
        pltpu.VMEM((rows * step, 128), f32),
        pltpu.VMEM((rows * step, width), bf16),
        pltpu.VMEM((count, 2 * spots), f32),
        pltpu.VMEM((2, rows, inner), bf16),
        pltpu.VMEM((2 * rows, inner), f32),
        pltpu.VMEM((inner, 2 * spots), bf16),
        pltpu.VMEM((rows, 2 * width), f32),
        pltpu.VMEM((rows, width), bf16),
        pltpu.VMEM((rows, width), bf16),
        pltpu.VMEM((rows, inner), bf16),
        pltpu.VMEM((rows, inner), bf16),
        pltpu.SemaphoreType.DMA((len(args),)),
        pltpu.SemaphoreType.DMA((11,)),
        pltpu.SemaphoreType.DMA((6, 4)),
    ]
    refined, errors = pl.pallas_call(
        functools.partial(kernel, n, heads),
        out_shape=(pltpu.VMEM((rows, inner), bf16), pltpu.VMEM((rows, count), f32)),
        in_specs=[pl.BlockSpec(memory_space=pltpu.HBM)] * len(args),
        out_specs=[pl.BlockSpec(memory_space=pltpu.VMEM)] * 2,
        scratch_shapes=scratch,
        compiler_params=pltpu.CompilerParams(
            collective_id=0, has_side_effects=True, vmem_limit_bytes=40 * 1024 * 1024),
        name="confidence",
    )(*[pltpu.with_memory_space_constraint(a, pltpu.HBM) for a in args])
    return pl.pallas_call(
        place,
        out_shape=(
            jax.ShapeDtypeStruct((rows, inner), bf16),
            jax.ShapeDtypeStruct((rows, count), f32),
        ),
        in_specs=[pl.BlockSpec(memory_space=pltpu.VMEM)] * 2,
        out_specs=[pl.BlockSpec(memory_space=pltpu.HBM)] * 2,
        scratch_shapes=[pltpu.SemaphoreType.DMA((2,))],
        compiler_params=pltpu.CompilerParams(vmem_limit_bytes=1024 * 1024),
        name="place",
    )(refined, errors)


def solution(mesh):
    placed = (
        P("groups", "rows", None),
        P(("groups", "rows"), None),
        P("groups"),
        P("groups"),
        P("groups"),
        P("groups"),
    ) + (P(),) * 14
    return jax.shard_map(
        functools.partial(on_device, mesh.shape["rows"]),
        mesh=mesh,
        in_specs=placed,
        out_specs=(P(("groups", "rows"), None), P(("groups", "rows"), None)),
        check_vma=False,
    )
```
